32 devices in a mesh: grp: 2 (over core), tile: 16 (over z, y, x).
Axes of the slice: x: 2, y: 2, z: 4, core: 2. Of those that a mesh axis runs over, the one named last changes fastest.
Arguments:
- source_points: float32 [2, 3, 524288], P('grp', None, 'tile'), may hold values from -6 to 6
- intersection: int32 [2, 2048, 1], P('grp', 'tile'), may hold values from 0 to 15; in each aligned block of 128 rows (0 to 127, 128 to 255, ..., all dimensions but the last counted through in order) at most 16 rows name the same one
- target_scan: int32 [2, 2048], P('grp', 'tile'), may hold values from 0 to 63
- matches: int32 [2, 524288], P('grp', 'tile'), may hold values from 0 to 511
- target_points: float32 [3, 524288], P(None, 'tile'), may hold values from -6 to 6
- target_normals: float32 [3, 524288], P(None, 'tile'), may hold values from -4 to 4
Outputs:
- pose_step: float32 [6, 1024], P(None, 'tile')
The draws below stay inside these ranges and needn't reach their ends.
Inputs may be any that keep to these rules, and one draw needn't show every extreme that they name: `intersection`: within the blocks of one device (each aligned run of 128 rows), no index is named more than 16 times, a bound that some block reaches.
All inputs are finite; a program needn't handle non-finite values.
Results may differ from the reference program's by a relative error of at most 0.0003.
Values sent between devices are 32-bit elements; how exact they have to be, the bound alone decides.
A program may use at most 64 MiB of HBM per device.

```python
import math
import jax
import jax.numpy as jnp
import numpy as np
from jax import lax

BLOCK_PTS = 256
BLOCKS_DEV = 128
SCANS_DEV = 64
TARGET_PTS = 512
CAP = 16
GRPS = 2
BLOCKS = 2048
SCANS = 1024
TILE_PTS = 524288
N_TILE = 16


def set_ends(array, stream_key, least, top_value):
    longest = array.shape.index(max(array.shape))
    spots = []
    for shift in (0, 1):
        where = [jax.random.randint(jax.random.fold_in(stream_key, axis), (), 0, length) for axis, length in enumerate(array.shape)]
        where[longest] = (where[longest] + shift) % array.shape[longest]
        spots.append(tuple(where))
    return array.at[spots[0]].set(least).at[spots[1]].set(top_value)


def shard_levels(stream_key, shape, shards, smallest, high):
    def one(axis_at, parts):
        steps = jax.random.uniform(jax.random.fold_in(jax.random.fold_in(stream_key, 6), axis_at), (parts,), jnp.float32, smallest / len(shards), high / len(shards))
        return jnp.repeat(jnp.exp(steps), shape[axis_at] // parts).reshape((-1,) + (1,) * (len(shape) - axis_at - 1))

    level = one(*shards[0])
    for cut in shards[1:]:
        level = level * one(*cut)
    return level


def routed_block(own_key, own, number, rows, amount, top, limit, skew):
    order = jax.random.permutation(own_key, amount)
    crowded, usual = shares(amount, rows * top, limit, skew, True), shares(amount, rows * top, limit, skew, False)
    places = jnp.arange(amount)

    def named(tallies, rotation):
        used = int((tallies > 0).sum())
        fixed = max(1, used // 4)
        passed = fixed + (places - fixed + rotation * (used - fixed)) % max(1, amount - fixed)
        return jnp.zeros((amount,), jnp.int32).at[order[jnp.where(places < fixed, places, passed)]].set(jnp.asarray(tallies, jnp.int32))

    tallies = jnp.where(number % 4 == 0, named(crowded, number // 4), named(usual, number - number // 4 - 1))
    mixed = jax.random.permutation(jax.random.fold_in(own, 3), amount)
    source_of, sink = mixed[0:amount // 2 * 2:2], mixed[1:amount // 2 * 2:2]
    slack = jnp.minimum(tallies[source_of] - 1, limit - tallies[sink]) // 2
    slack = jnp.where((source_of == order[0]) | (sink == order[0]) | (tallies[sink] == 0), 0, jnp.maximum(slack, 0))
    passed = jax.random.randint(jax.random.fold_in(own, 4), (amount // 2,), 0, 1 << 20) % (slack + 1)
    tallies = tallies.at[source_of].add(-passed).at[sink].add(passed)
    members = jnp.searchsorted(jnp.cumsum(tallies), jnp.arange(rows * top), side="right").astype(jnp.int32)
    grid = members.reshape(top, rows).T
    grid = grid[jax.random.permutation(jax.random.fold_in(own, 1), rows)]
    rotation = jax.random.randint(jax.random.fold_in(own, 2), (rows, 1), 0, top)
    return jnp.take_along_axis(grid, (jnp.arange(top)[None, :] + rotation) % top, axis=1)


def shares(amount, total, most, lean, full):
    loads = [(1 << 20) // math.isqrt(grade ** lean) + 1 for grade in range(1, amount + 1)]
    largest = most if full else min(most, max(-(-total // amount), total * loads[0] // sum(loads)))
    least = 1 if total - largest >= amount - 1 else 0
    given, spare = [largest] + [least] * (amount - 1), total - largest - least * (amount - 1)
    while spare > 0:
        movable = [i for i in range(1, amount) if given[i] < largest] or [i for i in range(1, amount) if given[i] < most]
        pool, left = sum([loads[i] for i in movable]), spare
        for i in movable:
            more = min(most - given[i], max(1, left * loads[i] // pool), spare)
            given[i] = given[i] + more
            spare = spare - more
    return np.array(given)


def gaussian(key, extent, width, reach, pieces=(), kind=jnp.bfloat16):
    drawn = jax.random.normal(key, extent, jnp.float32) * width
    if len(pieces) > 0:
        drawn = shard_levels(key, extent, pieces, -0.22, 0.18) * drawn
    return jnp.clip(drawn, min=-reach, max=reach).astype(kind)


def setup_inputs(seed: int = 0) -> dict:
    keys = jax.random.split(jax.random.key(seed), 7)
    source_points = gaussian(keys[0], (GRPS, 3, BLOCKS * BLOCK_PTS), 1.0, 6.0, ((0, 2), (2, 16)), jnp.float32)
    intersection_keys = jax.random.split(jax.random.fold_in(keys[1], 1), GRPS * BLOCKS // BLOCKS_DEV)
    intersection_turns = jax.random.permutation(jax.random.fold_in(keys[1], 3), GRPS * BLOCKS // BLOCKS_DEV)
    intersection = jax.vmap(lambda own, number: routed_block(jax.random.fold_in(keys[1], 2), own, number, BLOCKS_DEV, N_TILE, 1, CAP, 2))(intersection_keys, intersection_turns).reshape((GRPS, BLOCKS, 1))
    target_scan = set_ends(jax.random.randint(keys[2], (GRPS, BLOCKS), 0, SCANS_DEV), jax.random.fold_in(keys[2], 1), 0, SCANS_DEV - 1).astype(jnp.int32)
    matches = set_ends(jax.random.randint(keys[3], (GRPS, BLOCKS * BLOCK_PTS), 0, TARGET_PTS), jax.random.fold_in(keys[3], 1), 0, TARGET_PTS - 1).astype(jnp.int32)
    target_points = gaussian(keys[4], (3, TILE_PTS), 1.0, 6.0, ((1, 16),), jnp.float32)
    target_normals = gaussian(keys[5], (3, TILE_PTS), 0.6, 4.0, ((1, 16),), jnp.float32)
    return {"source_points": source_points, "intersection": intersection, "target_scan": target_scan, "matches": matches, "target_points": target_points, "target_normals": target_normals}


DAMPING = 0.1
PRECISE = lax.Precision.HIGHEST


def cross_rows(first_vec, second_vec):
    return jnp.stack([first_vec[1] * second_vec[2] - first_vec[2] * second_vec[1],
                      first_vec[2] * second_vec[0] - first_vec[0] * second_vec[2],
                      first_vec[0] * second_vec[1] - first_vec[1] * second_vec[0]])


def pair_terms(source, target, normal, usable):
    jacobian = jnp.concatenate([cross_rows(source, normal), normal, -cross_rows(target, normal), -normal], axis=0) * usable[None]
    misfit = jnp.sum(normal * (source - target), axis=0) * usable
    normal_blocks = jnp.einsum("anks,bnks->abnk", jacobian, jacobian, precision=PRECISE)
    gradient = jnp.einsum("anks,nks->ank", jacobian, misfit, precision=PRECISE)
    layout = jacobian.shape[1:3]
    own_terms = jnp.concatenate([normal_blocks[:6, :6].reshape((36,) + layout), gradient[:6]], axis=0)
    theirs = jnp.concatenate([normal_blocks[6:, 6:].reshape((36,) + layout), gradient[6:]], axis=0)
    return own_terms, theirs


def solve_poses(scan_totals):
    entries = [[scan_totals[6 * row_at + col_at] for col_at in range(6)] for row_at in range(6)]
    traced = entries[0][0]
    for step_at in range(1, 6):
        traced = traced + entries[step_at][step_at]
    shift_by = DAMPING * traced / 6.0
    for step_at in range(6):
        entries[step_at][step_at] = entries[step_at][step_at] + shift_by
    values = [-scan_totals[36 + row_at] for row_at in range(6)]
    for pivot_at in range(6):
        for row_at in range(pivot_at + 1, 6):
            factor = entries[row_at][pivot_at] / entries[pivot_at][pivot_at]
            for col_at in range(pivot_at, 6):
                entries[row_at][col_at] = entries[row_at][col_at] - factor * entries[pivot_at][col_at]
            values[row_at] = values[row_at] - factor * values[pivot_at]
    result = [None] * 6
    for row_at in range(5, -1, -1):
        running = values[row_at]
        for col_at in range(row_at + 1, 6):
            running = running - entries[row_at][col_at] * result[col_at]
        result[row_at] = running / entries[row_at][row_at]
    return jnp.stack(result)


def reference(source_points, intersection, target_scan, matches, target_points, target_normals):
    per_scan = BLOCKS_DEV // SCANS_DEV
    block_span = BLOCKS_DEV * BLOCK_PTS
    tile_span = SCANS_DEV * TARGET_PTS
    anchor = jnp.int32(0)

    def accumulate(totals, stretch_at):
        grp_at = (stretch_at // N_TILE).astype(jnp.int32)
        tile_at = (stretch_at % N_TILE).astype(jnp.int32)
        coords = lax.dynamic_slice(source_points, (grp_at, anchor, tile_at * block_span), (1, 3, block_span))[0]
        coords = coords.reshape(3, 1, BLOCKS_DEV, BLOCK_PTS)
        destin = lax.dynamic_slice(intersection, (grp_at, tile_at * BLOCKS_DEV, anchor), (1, BLOCKS_DEV, 1))[0, :, 0]
        chosen = lax.dynamic_slice(target_scan, (grp_at, tile_at * BLOCKS_DEV), (1, BLOCKS_DEV))[0]
        picked = lax.dynamic_slice(matches, (grp_at, tile_at * block_span), (1, block_span))[0].reshape(BLOCKS_DEV, BLOCK_PTS)
        target_index = (destin[:, None] * tile_span + chosen[:, None] * TARGET_PTS + picked).astype(jnp.int32)
        nearest = jnp.take(target_points, target_index, axis=1)[:, None]
        facing = jnp.take(target_normals, target_index, axis=1)[:, None]
        usable = jnp.ones((1, BLOCKS_DEV, BLOCK_PTS), jnp.float32)
        own_terms, theirs = pair_terms(coords, nearest, facing, usable)
        source_ids = (tile_at * SCANS_DEV + jnp.arange(BLOCKS_DEV, dtype=jnp.int32) // per_scan).astype(jnp.int32)
        target_ids = (destin * SCANS_DEV + chosen).astype(jnp.int32)
        totals = totals + jax.ops.segment_sum(own_terms[:, 0].T, source_ids, num_segments=SCANS).T
        totals = totals + jax.ops.segment_sum(theirs[:, 0].T, target_ids, num_segments=SCANS).T
        return totals, None

    totals, unused = lax.scan(accumulate, jnp.zeros((42, SCANS), jnp.float32), jnp.arange(GRPS * N_TILE, dtype=jnp.int32))
    return solve_poses(totals)
```

```python
import jax
import jax.numpy as jnp
from jax import lax
from jax.experimental import pallas as pl
from jax.experimental.pallas import tpu as pltpu
from jax.sharding import PartitionSpec as P

SCANS_DEV = 64
TARGET_PTS = 512
DAMPING = 0.1
LANES = 128
PAIR = 32
AHEAD = 4
PRECISE = lax.Precision.HIGHEST
MESH = pl.DeviceIdType.MESH
VMEM = pl.BlockSpec(memory_space=pltpu.VMEM)
ANY = pl.BlockSpec(memory_space=pl.ANY)


def plan(dest, chosen, block, ids, seg):
    tiles = ids.shape[0]
    blocks = dest.shape[1]
    cap = seg.shape[0] * 8
    per_scan = blocks // SCANS_DEV
    f32 = jnp.float32
    hit = dest[...] == lax.broadcasted_iota(jnp.int32, (tiles, blocks), 0)
    first = lax.broadcasted_iota(jnp.int32, (blocks, blocks), 0)
    second = lax.broadcasted_iota(jnp.int32, (blocks, blocks), 1)
    rank = jnp.dot(
        hit.astype(f32), (first <= second).astype(f32), preferred_element_type=f32
    ).astype(jnp.int32)
    rank = jnp.where(hit, rank, 0)
    place = lax.broadcasted_iota(jnp.int32, (tiles, blocks), 1).astype(f32) + 1.0
    wanted = chosen[...].astype(f32) + 1.0
    lane = lax.broadcasted_iota(jnp.int32, (tiles, LANES), 1)
    at = jnp.zeros((tiles, LANES), f32)
    named = jnp.zeros((tiles, LANES), f32)
    for r in range(cap):
        mine = rank == r + 1
        at = jnp.where(
            lane == r, jnp.sum(jnp.where(mine, place, 0.0), axis=1, keepdims=True), at
        )
        named = jnp.where(
            lane == r, jnp.sum(jnp.where(mine, wanted, 0.0), axis=1, keepdims=True), named
        )
    at = at.astype(jnp.int32) - 1
    named = named.astype(jnp.int32) - 1
    block[...] = at
    scan = jnp.where(at >= 0, at // per_scan, -1)
    for t in range(tiles):
        ids[t] = named[t : t + 1]
    for g in range(cap // 8):
        seg[g : g + 1, :] = jnp.concatenate(
            [scan[t : t + 1, g * 8 : g * 8 + 8] for t in range(tiles)], axis=1
        )


def flip(me, k, tiles):
    other, bit = 0, 1
    while bit < tiles:
        other = other + (me // bit + k // bit) % 2 * bit
        bit *= 2
    return other


def partner_at(j, me, tiles):
    odd = j % 2
    k = odd * (tiles - (j + 1) // 2) + (1 - odd) * (tiles // 2 - j // 2) * jnp.minimum(j, 1)
    return flip(me, k, tiles)


def cross(u, v):
    return [
        u[1] * v[2] - u[2] * v[1],
        u[2] * v[0] - u[0] * v[2],
        u[0] * v[1] - u[1] * v[0],
    ]


def upper(vec):
    return [(a, b) for a in range(6) for b in range(a, 6)]


def main_kernel(
    dest_in, chosen_in, sp_in, mt_in, tp_in, tn_in, out,
    dest, chosen, sp, mt, tp, tn, places, block, ids, seg,
    pts, idx, got_pts, got_idx, got_ids, named, table, picked, own, far, back, tot, partner,
    ps, pr, qs, qr, js, jr, ss, rs, ls, gs, gr,
):
    tiles, _, cap, points = pts.shape
    blocks = dest.shape[1]
    me = lax.axis_index("tile")
    other = 1 - lax.axis_index("grp")
    barrier = pltpu.get_barrier_semaphore()

    def greet(k, c):
        to = lax.rem(me + k, tiles)
        pl.semaphore_signal(barrier, inc=1, device_id={"tile": to}, device_id_type=MESH)
        return c

    lax.fori_loop(1, tiles, greet, 0)
    pl.semaphore_signal(barrier, inc=1, device_id={"grp": other}, device_id_type=MESH)
    loads = [
        pltpu.make_async_copy(src, dst, ls.at[i])
        for i, (src, dst) in enumerate(
            [(dest_in, dest), (chosen_in, chosen), (sp_in, sp), (mt_in, mt), (tp_in, tp), (tn_in, tn)]
        )
    ]
    for load in loads:
        load.start()

    def remote(src, dst, send, recv, to, frm):
        return pltpu.make_async_remote_copy(
            src.at[to], dst.at[frm], send.at[to], recv.at[frm], {"tile": to}, MESH
        )

    def id_copy(to, frm):
        return remote(ids, got_ids, js, jr, to, frm)

    def idx_copy(to, frm):
        return remote(idx, got_idx, qs, qr, to, frm)

    def pts_copy(to, frm):
        return remote(pts, got_pts, ps, pr, to, frm)

    def own_copy(to, frm):
        return remote(own, back, ss, rs, to, frm)

    def each(start, stop, act):
        def one(j, c):
            act(partner_at(j, me, tiles), j)
            return c

        lax.fori_loop(start, stop, one, 0)

    def pack(t, pts_to, idx_to):
        for r in range(cap):
            b = block[t, r]
            used = jnp.minimum(b, 0) + 1
            for h in range(points // LANES):
                span = slice(h * LANES, (h + 1) * LANES)
                at = jnp.clip(b, 0, blocks - 1) * (points // LANES) + h
                for a in range(3):
                    pts_to[t, a, r : r + 1, span] = sp[a, at]
                idx_to[t, r : r + 1, span] = mt[at] * used + (used - 1)

    def send(t):
        idx_copy(t, me).start()
        pts_copy(t, me).start()

    loads[0].wait()
    loads[1].wait()
    plan(dest, chosen, places, ids, seg)
    to_smem = pltpu.make_async_copy(places, block, ls.at[6])
    to_smem.start()
    loads[2].wait()
    loads[3].wait()
    to_smem.wait()
    ahead = min(AHEAD, tiles - 1)
    each(1, ahead + 1, lambda t, j: pack(t, pts, idx))
    pl.semaphore_wait(barrier, tiles)
    each(1, tiles, lambda t, j: id_copy(t, me).start())
    each(1, ahead + 1, lambda t, j: send(t))

    def pack_send(t, j):
        @pl.when(j < tiles)
        def _():
            pack(t, pts, idx)

        @pl.when(j > ahead + 1)
        def _():
            send(partner_at(j - 1, me, tiles))

    each(ahead + 1, tiles + 1, pack_send)
    self_ids = pltpu.make_async_copy(ids.at[me], got_ids.at[me], ls.at[7])
    self_ids.start()
    pack(me, got_pts, got_idx)
    loads[4].wait()
    loads[5].wait()

    def fill(s, c):
        cols = pl.ds(pl.multiple_of(s * TARGET_PTS, TARGET_PTS), TARGET_PTS)
        table[s, 0:3, :] = tp[:, cols]
        table[s, 3:6, :] = tn[:, cols]
        return c

    lax.fori_loop(0, SCANS_DEV, fill, 0, unroll=4)
    tot[...] = jnp.zeros(tot.shape, jnp.float32)
    self_ids.wait()
    each(1, tiles, lambda t, j: id_copy(t, t).wait_recv())
    load_ids = pltpu.make_async_copy(got_ids, named, ls.at[8])
    load_ids.start()
    load_ids.wait()
    lane = lax.broadcasted_iota(jnp.int32, (8, LANES), 1)
    scan = lax.broadcasted_iota(jnp.int32, (SCANS_DEV, cap), 0)

    def group(d, g):
        r0 = g * 8
        near = got_idx[d, r0 : r0 + 8, :]
        for j in range(8):
            tab = table.at[jnp.clip(named[d, 0, r0 + j], 0, SCANS_DEV - 1)]
            for h in range(points // LANES):
                at = jnp.broadcast_to(near[j : j + 1, h * LANES : (h + 1) * LANES], (8, LANES))
                low = at & (LANES - 1)
                high = (at >> 7) & (TARGET_PTS // LANES - 1)
                res = None
                for q in range(TARGET_PTS // LANES):
                    part = jnp.take_along_axis(
                        tab[:, q * LANES : (q + 1) * LANES],
                        low,
                        axis=1,
                        mode="promise_in_bounds",
                    )
                    res = part if res is None else jnp.where(high == q, part, res)
                picked[g, h, j * 8 : j * 8 + 8, :] = res
        halves = []
        for h in range(points // LANES):
            span = slice(h * LANES, (h + 1) * LANES)
            good = near[:, span] >= 0
            p = [
                jnp.where(good, got_pts[d, a, r0 : r0 + 8, span], 0.0) for a in range(3)
            ]
            q = [picked[g, h, pl.ds(a, 8, stride=8), :] for a in range(3)]
            n = [
                jnp.where(good, picked[g, h, pl.ds(3 + a, 8, stride=8), :], 0.0)
                for a in range(3)
            ]
            mis = n[0] * (p[0] - q[0]) + n[1] * (p[1] - q[1]) + n[2] * (p[2] - q[2])
            halves.append((cross(p, n) + n, cross(q, n) + n, mis))
        own_row = jnp.zeros((8, LANES), jnp.float32)
        far_row = jnp.zeros((8, LANES), jnp.float32)

        def total(make):
            acc = None
            for half in halves:
                acc = make(half) if acc is None else acc + make(half)
            return jnp.sum(acc, axis=1, keepdims=True)

        for f, (a, b) in enumerate(upper(6)):
            s = total(lambda v: v[0][a] * v[0][b])
            own_row = jnp.where(lane == PAIR * g + f, s, own_row)
            if a < 3:
                s = total(lambda v: v[1][a] * v[1][b])
            far_row = jnp.where(lane == f, s, far_row)
        for a in range(6):
            s = total(lambda v: v[0][a] * v[2])
            own_row = jnp.where(lane == PAIR * g + 21 + a, s, own_row)
            if a < 3:
                s = total(lambda v: v[1][a] * v[2])
            far_row = jnp.where(lane == 21 + a, -s, far_row)
        far[r0 : r0 + 8, :] = far_row
        return own_row

    def work(t, j):
        @pl.when(j > 0)
        def _():
            idx_copy(t, t).wait_recv()
            pts_copy(t, t).wait_recv()

        row = group(t, 0)
        for g in range(1, cap // 8):
            row = row + group(t, g)
        own[t] = row

        @pl.when(j == 0)
        def _():
            back[me] = own[me]

        @pl.when(j > 0)
        def _():
            own_copy(t, me).start()

        here = (scan == got_ids[t][:, :cap]).astype(jnp.float32)
        tot[...] += jnp.dot(
            here, far[...], precision=PRECISE, preferred_element_type=jnp.float32
        )

    each(0, tiles, work)
    each(1, tiles, lambda t, j: own_copy(t, t).wait_recv())
    wide = lax.broadcasted_iota(jnp.int32, (SCANS_DEV, tiles * 8), 0)
    rows = back[...].reshape(tiles * 8, LANES)
    sums = tot[...]
    for g in range(cap // 8):
        here = (wide == seg[g : g + 1, :]).astype(jnp.float32)
        part = jnp.dot(here, rows, precision=PRECISE, preferred_element_type=jnp.float32)
        if g > 0:
            part = pltpu.roll(part, LANES - PAIR * g, 1)
        sums = sums + part
    tot[...] = sums
    swap = pltpu.make_async_remote_copy(tot, partner, gs, gr, {"grp": other}, MESH)
    swap.start()

    def drain(t, j):
        for copy in (id_copy, idx_copy, pts_copy, own_copy):
            copy(t, me).wait_send()

    each(1, tiles, drain)
    swap.wait()
    full = jnp.transpose(tot[...] + partner[...])
    for a, row in enumerate(solve_rows([full[f : f + 1, :] for f in range(27)])):
        out[a : a + 1, :] = row


def solve_rows(rows):
    entries = {}
    for f, (a, b) in enumerate(upper(6)):
        entries[a, b] = rows[f]
    traced = entries[0, 0]
    for a in range(1, 6):
        traced = traced + entries[a, a]
    shift_by = DAMPING * traced / 6.0
    for a in range(6):
        entries[a, a] = entries[a, a] + shift_by
    values = [-rows[21 + a] for a in range(6)]
    for k in range(6):
        for a in range(k + 1, 6):
            factor = entries[k, a] / entries[k, k]
            for b in range(a, 6):
                entries[a, b] = entries[a, b] - factor * entries[k, b]
            values[a] = values[a] - factor * values[k]
    result = [None] * 6
    for a in range(5, -1, -1):
        running = values[a]
        for b in range(a + 1, 6):
            running = running - entries[a, b] * result[b]
        result[a] = running / entries[a, a]
    return result


def body(source_points, intersection, target_scan, matches, target_points, target_normals):
    tiles = lax.axis_size("tile")
    blocks = intersection.shape[1]
    points = source_points.shape[2] // blocks
    cap = -(-(2 * blocks // tiles) // 8) * 8
    f32, i32 = jnp.float32, jnp.int32
    shape = jax.ShapeDtypeStruct
    many = pltpu.SemaphoreType.DMA((tiles,))
    pts_t, idx_t = (tiles, 3, cap, points), (tiles, cap, points)
    rows = (3, blocks * points // LANES, 1, LANES)
    ids_t, sums_t = (tiles, 1, LANES), (SCANS_DEV, LANES)
    return pl.pallas_call(
        main_kernel,
        out_shape=shape((6, SCANS_DEV), f32),
        in_specs=[ANY] * 6,
        out_specs=VMEM,
        scratch_shapes=[
            pltpu.VMEM((1, blocks), i32),
            pltpu.VMEM((1, blocks), i32),
            pltpu.VMEM(rows, f32),
            pltpu.VMEM(rows[1:], i32),
            pltpu.VMEM(target_points.shape, f32),
            pltpu.VMEM(target_normals.shape, f32),
            pltpu.VMEM((tiles, LANES), i32),
            pltpu.SMEM((tiles, LANES), i32),
            pltpu.VMEM(ids_t, i32),
            pltpu.VMEM((cap // 8, tiles * 8), i32),
            pltpu.VMEM(pts_t, f32),
            pltpu.VMEM(idx_t, i32),
            pltpu.VMEM(pts_t, f32),
            pltpu.VMEM(idx_t, i32),
            pltpu.VMEM(ids_t, i32),
            pltpu.SMEM(ids_t, i32),
            pltpu.VMEM((SCANS_DEV, 8, TARGET_PTS), f32),
            pltpu.VMEM((cap // 8, points // LANES, 64, LANES), f32),
            pltpu.VMEM((tiles, 8, LANES), f32),
            pltpu.VMEM((cap, LANES), f32),
            pltpu.VMEM((tiles, 8, LANES), f32),
            pltpu.VMEM(sums_t, f32),
            pltpu.VMEM(sums_t, f32),
        ]
        + [many] * 8
        + [pltpu.SemaphoreType.DMA((9,)), pltpu.SemaphoreType.DMA, pltpu.SemaphoreType.DMA],
        compiler_params=pltpu.CompilerParams(collective_id=0, has_side_effects=True),
        name="main",
    )(
        intersection.reshape(1, blocks),
        target_scan,
        source_points.reshape(rows),
        matches.reshape(rows[1:]),
        target_points,
        target_normals,
    )


def solution(mesh):
    in_specs = (
        P("grp", None, "tile"),
        P("grp", "tile", None),
        P("grp", "tile"),
        P("grp", "tile"),
        P(None, "tile"),
        P(None, "tile"),
    )
    out_specs = P(None, "tile")
    return jax.shard_map(body, mesh=mesh, in_specs=in_specs, out_specs=out_specs, check_vma=False)
```

```python
import jax
import jax.numpy as jnp
from jax import lax
from jax.experimental import pallas as pl
from jax.experimental.pallas import tpu as pltpu
from jax.sharding import PartitionSpec as P

SCANS_DEV = 64
TARGET_PTS = 512
DAMPING = 0.1
LANES = 128
PAIR = 32
AHEAD = 4
PRECISE = lax.Precision.HIGHEST
MESH = pl.DeviceIdType.MESH
VMEM = pl.BlockSpec(memory_space=pltpu.VMEM)
ANY = pl.BlockSpec(memory_space=pl.ANY)


def plan(dest, chosen, block, ids, seg):
    tiles = ids.shape[0]
    blocks = dest.shape[1]
    cap = seg.shape[0] * 8
    per_scan = blocks // SCANS_DEV
    f32 = jnp.float32
    hit = dest[...] == lax.broadcasted_iota(jnp.int32, (tiles, blocks), 0)
    first = lax.broadcasted_iota(jnp.int32, (blocks, blocks), 0)
    second = lax.broadcasted_iota(jnp.int32, (blocks, blocks), 1)
    rank = jnp.dot(
        hit.astype(f32), (first <= second).astype(f32), preferred_element_type=f32
    ).astype(jnp.int32)
    rank = jnp.where(hit, rank, 0)
    place = lax.broadcasted_iota(jnp.int32, (tiles, blocks), 1).astype(f32) + 1.0
    wanted = chosen[...].astype(f32) + 1.0
    lane = lax.broadcasted_iota(jnp.int32, (tiles, LANES), 1)
    at = jnp.zeros((tiles, LANES), f32)
    named = jnp.zeros((tiles, LANES), f32)
    for r in range(cap):
        mine = rank == r + 1
        at = jnp.where(
            lane == r, jnp.sum(jnp.where(mine, place, 0.0), axis=1, keepdims=True), at
        )
        named = jnp.where(
            lane == r, jnp.sum(jnp.where(mine, wanted, 0.0), axis=1, keepdims=True), named
        )
    at = at.astype(jnp.int32) - 1
    named = named.astype(jnp.int32) - 1
    block[...] = at
    scan = jnp.where(at >= 0, at // per_scan, -1)
    for t in range(tiles):
        ids[t] = named[t : t + 1]
    for g in range(cap // 8):
        seg[g : g + 1, :] = jnp.concatenate(
            [scan[t : t + 1, g * 8 : g * 8 + 8] for t in range(tiles)], axis=1
        )


def flip(me, k, tiles):
    other, bit = 0, 1
    while bit < tiles:
        other = other + (me // bit + k // bit) % 2 * bit
        bit *= 2
    return other


def send_at(j, me, tiles):
    half, quarter = tiles // 2, tiles // 4
    i = j // 2
    far = (3 - i % 2) * quarter + quarter - 1 - i // 2
    return flip(me, jnp.where(j % 2 == 1, far, half - i), tiles)


def recv_at(j, me, tiles):
    half, quarter = tiles // 2, tiles // 4
    place = me // quarter
    inner = (place // 2 + place) % 2
    last = j // (tiles - 1)
    i = j // 2 - 1 + last
    second = i // quarter
    code = 3 - (inner + second) % 2
    far = code * quarter + quarter - 1 - i % quarter
    near = (half - (j + 1) // 2) * jnp.minimum(j, 1)
    return flip(me, jnp.where((j > 0) & (j % 2 - last == 0), far, near), tiles)


def cross(u, v):
    return [
        u[1] * v[2] - u[2] * v[1],
        u[2] * v[0] - u[0] * v[2],
        u[0] * v[1] - u[1] * v[0],
    ]


def upper(vec):
    return [(a, b) for a in range(6) for b in range(a, 6)]


def main_kernel(
    dest_in, chosen_in, sp_in, mt_in, tp_in, tn_in, out,
    dest, chosen, sp, mt, tp, tn, places, block, ids, seg,
    pts, idx, got_pts, got_idx, got_ids, named, table, picked, own, far, back, tot, partner,
    ps, pr, qs, qr, js, jr, ss, rs, ls, gs, gr,
):
    tiles, _, cap, points = pts.shape
    blocks = dest.shape[1]
    me = lax.axis_index("tile")
    other = 1 - lax.axis_index("grp")
    barrier = pltpu.get_barrier_semaphore()

    def greet(k, c):
        to = lax.rem(me + k, tiles)
        pl.semaphore_signal(barrier, inc=1, device_id={"tile": to}, device_id_type=MESH)
        return c

    lax.fori_loop(1, tiles, greet, 0)
    pl.semaphore_signal(barrier, inc=1, device_id={"grp": other}, device_id_type=MESH)
    loads = [
        pltpu.make_async_copy(src, dst, ls.at[i])
        for i, (src, dst) in enumerate(
            [(dest_in, dest), (chosen_in, chosen), (sp_in, sp), (mt_in, mt), (tp_in, tp), (tn_in, tn)]
        )
    ]
    for load in loads:
        load.start()

    def remote(src, dst, send, recv, to, frm):
        return pltpu.make_async_remote_copy(
            src.at[to], dst.at[frm], send.at[to], recv.at[frm], {"tile": to}, MESH
        )

    def id_copy(to, frm):
        return remote(ids, got_ids, js, jr, to, frm)

    def idx_copy(to, frm):
        return remote(idx, got_idx, qs, qr, to, frm)

    def pts_copy(to, frm):
        return remote(pts, got_pts, ps, pr, to, frm)

    def own_copy(to, frm):
        return remote(own, back, ss, rs, to, frm)

    def each(start, stop, act, at=send_at):
        def one(j, c):
            act(at(j, me, tiles), j)
            return c

        lax.fori_loop(start, stop, one, 0)

    def pack(t, pts_to, idx_to):
        for r in range(cap):
            b = block[t, r]
            used = jnp.minimum(b, 0) + 1
            for h in range(points // LANES):
                span = slice(h * LANES, (h + 1) * LANES)
                at = jnp.clip(b, 0, blocks - 1) * (points // LANES) + h
                for a in range(3):
                    pts_to[t, a, r : r + 1, span] = sp[a, at]
                idx_to[t, r : r + 1, span] = mt[at] * used + (used - 1)

    def send(t):
        idx_copy(t, me).start()
        pts_copy(t, me).start()

    loads[0].wait()
    loads[1].wait()
    plan(dest, chosen, places, ids, seg)
    to_smem = pltpu.make_async_copy(places, block, ls.at[6])
    to_smem.start()
    loads[2].wait()
    loads[3].wait()
    to_smem.wait()
    ahead = min(AHEAD, tiles - 1)
    each(1, ahead + 1, lambda t, j: pack(t, pts, idx))
    pl.semaphore_wait(barrier, tiles)
    each(1, tiles, lambda t, j: id_copy(t, me).start())
    each(1, ahead + 1, lambda t, j: send(t))

    def pack_send(t, j):
        @pl.when(j < tiles)
        def _():
            pack(t, pts, idx)

        @pl.when(j > ahead + 1)
        def _():
            send(send_at(j - 1, me, tiles))

    each(ahead + 1, tiles + 1, pack_send)
    self_ids = pltpu.make_async_copy(ids.at[me], got_ids.at[me], ls.at[7])
    self_ids.start()
    pack(me, got_pts, got_idx)
    loads[4].wait()
    loads[5].wait()

    def fill(s, c):
        cols = pl.ds(pl.multiple_of(s * TARGET_PTS, TARGET_PTS), TARGET_PTS)
        table[s, 0:3, :] = tp[:, cols]
        table[s, 3:6, :] = tn[:, cols]
        return c

    lax.fori_loop(0, SCANS_DEV, fill, 0, unroll=4)
    tot[...] = jnp.zeros(tot.shape, jnp.float32)
    self_ids.wait()
    each(1, tiles, lambda t, j: id_copy(t, t).wait_recv())
    load_ids = pltpu.make_async_copy(got_ids, named, ls.at[8])
    load_ids.start()
    load_ids.wait()
    lane = lax.broadcasted_iota(jnp.int32, (8, LANES), 1)
    scan = lax.broadcasted_iota(jnp.int32, (SCANS_DEV, cap), 0)

    def group(d, g):
        r0 = g * 8
        near = got_idx[d, r0 : r0 + 8, :]
        for j in range(8):
            tab = table.at[jnp.clip(named[d, 0, r0 + j], 0, SCANS_DEV - 1)]
            for h in range(points // LANES):
                at = jnp.broadcast_to(near[j : j + 1, h * LANES : (h + 1) * LANES], (8, LANES))
                low = at & (LANES - 1)
                high = (at >> 7) & (TARGET_PTS // LANES - 1)
                res = None
                for q in range(TARGET_PTS // LANES):
                    part = jnp.take_along_axis(
                        tab[:, q * LANES : (q + 1) * LANES],
                        low,
                        axis=1,
                        mode="promise_in_bounds",
                    )
                    res = part if res is None else jnp.where(high == q, part, res)
                picked[g, h, j * 8 : j * 8 + 8, :] = res
        halves = []
        for h in range(points // LANES):
            span = slice(h * LANES, (h + 1) * LANES)
            good = near[:, span] >= 0
            p = [
                jnp.where(good, got_pts[d, a, r0 : r0 + 8, span], 0.0) for a in range(3)
            ]
            q = [picked[g, h, pl.ds(a, 8, stride=8), :] for a in range(3)]
            n = [
                jnp.where(good, picked[g, h, pl.ds(3 + a, 8, stride=8), :], 0.0)
                for a in range(3)
            ]
            mis = n[0] * (p[0] - q[0]) + n[1] * (p[1] - q[1]) + n[2] * (p[2] - q[2])
            halves.append((cross(p, n) + n, cross(q, n) + n, mis))
        own_row = jnp.zeros((8, LANES), jnp.float32)
        far_row = jnp.zeros((8, LANES), jnp.float32)

        def total(make):
            acc = None
            for half in halves:
                acc = make(half) if acc is None else acc + make(half)
            return jnp.sum(acc, axis=1, keepdims=True)

        for f, (a, b) in enumerate(upper(6)):
            s = total(lambda v: v[0][a] * v[0][b])
            own_row = jnp.where(lane == PAIR * g + f, s, own_row)
            if a < 3:
                s = total(lambda v: v[1][a] * v[1][b])
            far_row = jnp.where(lane == f, s, far_row)
        for a in range(6):
            s = total(lambda v: v[0][a] * v[2])
            own_row = jnp.where(lane == PAIR * g + 21 + a, s, own_row)
            if a < 3:
                s = total(lambda v: v[1][a] * v[2])
            far_row = jnp.where(lane == 21 + a, -s, far_row)
        far[r0 : r0 + 8, :] = far_row
        return own_row

    def work(t, j):
        @pl.when(j > 0)
        def _():
            idx_copy(t, t).wait_recv()
            pts_copy(t, t).wait_recv()

        row = group(t, 0)
        for g in range(1, cap // 8):
            row = row + group(t, g)
        own[t] = row

        @pl.when(j == 0)
        def _():
            back[me] = own[me]

        @pl.when(j > 0)
        def _():
            own_copy(t, me).start()

        here = (scan == got_ids[t][:, :cap]).astype(jnp.float32)
        tot[...] += jnp.dot(
            here, far[...], precision=PRECISE, preferred_element_type=jnp.float32
        )

    each(0, tiles, work, recv_at)
    each(1, tiles, lambda t, j: own_copy(t, t).wait_recv())
    wide = lax.broadcasted_iota(jnp.int32, (SCANS_DEV, tiles * 8), 0)
    rows = back[...].reshape(tiles * 8, LANES)
    sums = tot[...]
    for g in range(cap // 8):
        here = (wide == seg[g : g + 1, :]).astype(jnp.float32)
        part = jnp.dot(here, rows, precision=PRECISE, preferred_element_type=jnp.float32)
        if g > 0:
            part = pltpu.roll(part, LANES - PAIR * g, 1)
        sums = sums + part
    tot[...] = sums
    swap = pltpu.make_async_remote_copy(tot, partner, gs, gr, {"grp": other}, MESH)
    swap.start()

    def drain(t, j):
        for copy in (id_copy, idx_copy, pts_copy, own_copy):
            copy(t, me).wait_send()

    each(1, tiles, drain)
    swap.wait()
    full = jnp.transpose(tot[...] + partner[...])
    for a, row in enumerate(solve_rows([full[f : f + 1, :] for f in range(27)])):
        out[a : a + 1, :] = row


def solve_rows(rows):
    entries = {}
    for f, (a, b) in enumerate(upper(6)):
        entries[a, b] = rows[f]
    traced = entries[0, 0]
    for a in range(1, 6):
        traced = traced + entries[a, a]
    shift_by = DAMPING * traced / 6.0
    for a in range(6):
        entries[a, a] = entries[a, a] + shift_by
    values = [-rows[21 + a] for a in range(6)]
    for k in range(6):
        for a in range(k + 1, 6):
            factor = entries[k, a] / entries[k, k]
            for b in range(a, 6):
                entries[a, b] = entries[a, b] - factor * entries[k, b]
            values[a] = values[a] - factor * values[k]
    result = [None] * 6
    for a in range(5, -1, -1):
        running = values[a]
        for b in range(a + 1, 6):
            running = running - entries[a, b] * result[b]
        result[a] = running / entries[a, a]
    return result


def body(source_points, intersection, target_scan, matches, target_points, target_normals):
    tiles = lax.axis_size("tile")
    blocks = intersection.shape[1]
    points = source_points.shape[2] // blocks
    cap = -(-(2 * blocks // tiles) // 8) * 8
    f32, i32 = jnp.float32, jnp.int32
    shape = jax.ShapeDtypeStruct
    many = pltpu.SemaphoreType.DMA((tiles,))
    pts_t, idx_t = (tiles, 3, cap, points), (tiles, cap, points)
    rows = (3, blocks * points // LANES, 1, LANES)
    ids_t, sums_t = (tiles, 1, LANES), (SCANS_DEV, LANES)
    return pl.pallas_call(
        main_kernel,
        out_shape=shape((6, SCANS_DEV), f32),
        in_specs=[ANY] * 6,
        out_specs=VMEM,
        scratch_shapes=[
            pltpu.VMEM((1, blocks), i32),
            pltpu.VMEM((1, blocks), i32),
            pltpu.VMEM(rows, f32),
            pltpu.VMEM(rows[1:], i32),
            pltpu.VMEM(target_points.shape, f32),
            pltpu.VMEM(target_normals.shape, f32),
            pltpu.VMEM((tiles, LANES), i32),
            pltpu.SMEM((tiles, LANES), i32),
            pltpu.VMEM(ids_t, i32),
            pltpu.VMEM((cap // 8, tiles * 8), i32),
            pltpu.VMEM(pts_t, f32),
            pltpu.VMEM(idx_t, i32),
            pltpu.VMEM(pts_t, f32),
            pltpu.VMEM(idx_t, i32),
            pltpu.VMEM(ids_t, i32),
            pltpu.SMEM(ids_t, i32),
            pltpu.VMEM((SCANS_DEV, 8, TARGET_PTS), f32),
            pltpu.VMEM((cap // 8, points // LANES, 64, LANES), f32),
            pltpu.VMEM((tiles, 8, LANES), f32),
            pltpu.VMEM((cap, LANES), f32),
            pltpu.VMEM((tiles, 8, LANES), f32),
            pltpu.VMEM(sums_t, f32),
            pltpu.VMEM(sums_t, f32),
        ]
        + [many] * 8
        + [pltpu.SemaphoreType.DMA((9,)), pltpu.SemaphoreType.DMA, pltpu.SemaphoreType.DMA],
        compiler_params=pltpu.CompilerParams(collective_id=0, has_side_effects=True),
        name="main",
    )(
        intersection.reshape(1, blocks),
        target_scan,
        source_points.reshape(rows),
        matches.reshape(rows[1:]),
        target_points,
        target_normals,
    )


def solution(mesh):
    in_specs = (
        P("grp", None, "tile"),
        P("grp", "tile", None),
        P("grp", "tile"),
        P("grp", "tile"),
        P(None, "tile"),
        P(None, "tile"),
    )
    out_specs = P(None, "tile")
    return jax.shard_map(body, mesh=mesh, in_specs=in_specs, out_specs=out_specs, check_vma=False)
```

```python
import jax
import jax.numpy as jnp
from jax import lax
from jax.experimental import pallas as pl
from jax.experimental.pallas import tpu as pltpu
from jax.sharding import PartitionSpec as P

SCANS_DEV = 64
TARGET_PTS = 512
DAMPING = 0.1
LANES = 128
PAIR = 32
AHEAD = 3
MESH = pl.DeviceIdType.MESH
VMEM = pl.BlockSpec(memory_space=pltpu.VMEM)
ANY = pl.BlockSpec(memory_space=pl.ANY)


def spread(to, rows, wide):
    for g in range(to.shape[0]):
        to[g : g + 1, :] = jnp.concatenate(
            [rows[t : t + 1, g * wide : (g + 1) * wide] for t in range(rows.shape[0])], axis=1
        )


def plan(dest, chosen, block, ids, seg):
    tiles = ids.shape[0]
    blocks = dest.shape[1]
    cap = seg.shape[0] * 4
    per_scan = blocks // SCANS_DEV
    f32 = jnp.float32
    hit = dest[...] == lax.broadcasted_iota(jnp.int32, (tiles, blocks), 0)
    first = lax.broadcasted_iota(jnp.int32, (blocks, blocks), 0)
    second = lax.broadcasted_iota(jnp.int32, (blocks, blocks), 1)
    rank = jnp.dot(
        hit.astype(f32), (first <= second).astype(f32), preferred_element_type=f32
    ).astype(jnp.int32)
    rank = jnp.where(hit, rank, 0)
    place = lax.broadcasted_iota(jnp.int32, (tiles, blocks), 1).astype(f32) + 1.0
    wanted = chosen[...].astype(f32) + 1.0
    lane = lax.broadcasted_iota(jnp.int32, (tiles, LANES), 1)
    at = jnp.zeros((tiles, LANES), f32)
    named = jnp.zeros((tiles, LANES), f32)
    for r in range(cap):
        mine = rank == r + 1
        at = jnp.where(
            lane == r, jnp.sum(jnp.where(mine, place, 0.0), axis=1, keepdims=True), at
        )
        named = jnp.where(
            lane == r, jnp.sum(jnp.where(mine, wanted, 0.0), axis=1, keepdims=True), named
        )
    at = at.astype(jnp.int32) - 1
    named = named.astype(jnp.int32) - 1
    spread(block, at, 8)
    scan = jnp.where(at >= 0, at // per_scan, -1)
    for t in range(tiles):
        ids[t] = named[t : t + 1]
    spread(seg, scan, 4)


def flip(me, k, tiles):
    other, bit = 0, 1
    while bit < tiles:
        other = other + (me // bit + k // bit) % 2 * bit
        bit *= 2
    return other


def send_at(j, me, tiles):
    half, quarter = tiles // 2, tiles // 4
    i = j // 2
    place = me // quarter
    inner = (place // 2 + place) % 2
    code = 3 - (inner * (1 - i // quarter) + (1 - inner) * (i % 2))
    low = inner * (i % quarter) + (1 - inner) * (i // 2)
    far = code * quarter + quarter - 1 - low
    return flip(me, jnp.where(j % 2 == 1, far, half - i), tiles)


def recv_at(j, me, tiles):
    half, quarter = tiles // 2, tiles // 4
    place = me // quarter
    inner = (place // 2 + place) % 2
    last = j // (tiles - 1)
    i = j // 2 - 1 + last
    second = i // quarter
    code = 3 - (inner + second) % 2
    far = code * quarter + quarter - 1 - i % quarter
    near = (half - (j + 1) // 2) * jnp.minimum(j, 1)
    return flip(me, jnp.where((j > 0) & (j % 2 - last == 0), far, near), tiles)


def pick(here, rows):
    bf16, f32 = jnp.bfloat16, jnp.float32
    parts = []
    for _ in range(3):
        parts.append(rows.astype(bf16))
        rows = rows - parts[-1].astype(f32)
    here = here.astype(f32).astype(bf16)
    return jnp.dot(
        jnp.concatenate([here] * 3, axis=1),
        jnp.concatenate(parts, axis=0),
        preferred_element_type=f32,
    )


def cross(u, v):
    return [
        u[1] * v[2] - u[2] * v[1],
        u[2] * v[0] - u[0] * v[2],
        u[0] * v[1] - u[1] * v[0],
    ]


def upper(vec):
    return [(a, b) for a in range(6) for b in range(a, 6)]


def main_kernel(
    dest_in, chosen_in, sp_in, mt_in, tp_in, tn_in, out,
    dest, chosen, sp, mt, tp, tn, places, block, ids, seg,
    seg_other, pts, got, got_ids, named, table, picked, own, far, back, tot, partner,
    pr, ps, js, jr, ss, rs, ls, hs, hr, gs, gr,
):
    tiles, _, cap, points = pts.shape
    blocks = dest.shape[1]
    me = lax.axis_index("tile")
    grp = lax.axis_index("grp")
    other = 1 - grp
    barrier = pltpu.get_barrier_semaphore()

    def greet(k, c):
        to = lax.rem(me + k, tiles)
        for side in range(2):
            pl.semaphore_signal(
                barrier, inc=1, device_id={"grp": side, "tile": to}, device_id_type=MESH
            )
        return c

    pl.semaphore_signal(barrier, inc=1, device_id={"grp": other}, device_id_type=MESH)
    lax.fori_loop(1, tiles, greet, 0)
    loads = [
        pltpu.make_async_copy(src, dst, ls.at[i])
        for i, (src, dst) in enumerate(
            [(dest_in, dest), (chosen_in, chosen), (sp_in, sp), (mt_in, mt), (tp_in, tp), (tn_in, tn)]
        )
    ]
    for load in loads:
        load.start()

    def remote(src, dst, send, recv, to, side=grp):
        return pltpu.make_async_remote_copy(
            src, dst, send, recv, {"grp": side, "tile": to}, MESH
        )

    def id_copy(t):
        return remote(ids.at[t], got_ids.at[me], js, jr, t)

    def pts_copy(to, frm):
        return remote(pts.at[to], got.at[frm], ps, pr.at[frm], to)

    def own_copy(t, side):
        return remote(own.at[t], back.at[grp * tiles + me], ss, rs, t, side)

    def all_of(src, dst, send, recv, count):
        span = pl.ds(0, count)
        return remote(src.at[span], dst.at[span], send, recv, me, other)

    seg_copy = remote(seg, seg_other, hs, hr, me, other)
    swap = remote(tot, partner, gs, gr, me, other)

    def each(start, stop, act, at=send_at):
        def one(j, c):
            act(at(j, me, tiles), j)
            return c

        lax.fori_loop(start, stop, one, 0)

    def pack(t, to, at_to):
        for r in range(cap):
            b = block[r // 8, t * 8 + r % 8]
            used = jnp.minimum(b, 0) + 1
            for h in range(points // LANES):
                span = slice(h * LANES, (h + 1) * LANES)
                at = jnp.clip(b, 0, blocks - 1) * (points // LANES) + h
                for a in range(3):
                    to[at_to, a, r : r + 1, span] = sp[a, at]
                to[at_to, 3, r : r + 1, span] = (mt[at] * used + (used - 1)).astype(jnp.float32)

    loads[0].wait()
    loads[1].wait()
    plan(dest, chosen, places, ids, seg)
    to_smem = pltpu.make_async_copy(places, block, ls.at[6])
    to_smem.start()
    loads[2].wait()
    loads[3].wait()
    to_smem.wait()
    ahead = min(AHEAD, tiles - 1)
    each(1, ahead + 1, lambda t, j: pack(t, pts, t))
    pl.semaphore_wait(barrier, 2 * tiles - 1)
    each(1, tiles, lambda t, j: id_copy(t).start())
    each(1, ahead + 1, lambda t, j: pts_copy(t, me).start())
    seg_copy.start()

    def pack_send(t, j):
        @pl.when(j < tiles)
        def _():
            pack(t, pts, t)

        @pl.when(j > ahead + 1)
        def _():
            pts_copy(send_at(j - 1, me, tiles), me).start()

    each(ahead + 1, tiles + 1, pack_send)
    self_ids = pltpu.make_async_copy(ids.at[me], got_ids.at[me], ls.at[7])
    self_ids.start()
    pack(me, got, me)
    loads[4].wait()
    loads[5].wait()

    chunks = TARGET_PTS // LANES - 1

    def fill(s, c):
        def cols(q):
            return pl.ds(pl.multiple_of(s * TARGET_PTS + q * LANES, LANES), LANES)

        for q in range(chunks):
            span = slice(q * LANES, (q + 1) * LANES)
            table[s, 0:3, span] = tp[:, cols(q)]
            table[s, 3:6, span] = tn[:, cols(q)]
            for r in range(2):
                ref, a = ((tp, 2 * q + r), (tn, 2 * q + r - 3))[2 * q + r > 2]
                table[s, 6 + r : 7 + r, span] = ref[a : a + 1, cols(chunks)]
        return c

    lax.fori_loop(0, SCANS_DEV, fill, 0, unroll=4)
    tot[...] = jnp.zeros(tot.shape, jnp.float32)
    self_ids.wait()
    all_of(ids, got_ids, js, jr, tiles - 1).wait_recv()
    load_ids = pltpu.make_async_copy(got_ids, named, ls.at[8])
    load_ids.start()
    load_ids.wait()
    lane = lax.broadcasted_iota(jnp.int32, (8, LANES), 1)
    scan = lax.broadcasted_iota(jnp.int32, (SCANS_DEV, cap), 0)
    halves_of = points // LANES

    def gather(d, g):
        r0 = g * 8
        near = got[d, 3, r0 : r0 + 8, :].astype(jnp.int32)
        for j in range(8):
            tab = table.at[jnp.clip(named[d, 0, r0 + j], 0, SCANS_DEV - 1)]
            for h in range(halves_of):
                at = jnp.broadcast_to(near[j : j + 1, h * LANES : (h + 1) * LANES], (8, LANES))
                low = at & (LANES - 1)
                for q in range(chunks):
                    picked[g, h, q, j * 8 : j * 8 + 8, :] = jnp.take_along_axis(
                        tab[:, q * LANES : (q + 1) * LANES],
                        low,
                        axis=1,
                        mode="promise_in_bounds",
                    )

    def group(d, g, far_to):
        r0 = g * 8
        near = got[d, 3, r0 : r0 + 8, :].astype(jnp.int32)
        halves = []
        for h in range(halves_of):
            span = slice(h * LANES, (h + 1) * LANES)
            good = near[:, span] >= 0
            chunk = (near[:, span] >> 7) & chunks
            rows = []
            for a in range(6):
                row = picked[g, h, a // 2, pl.ds(6 + a % 2, 8, stride=8), :]
                for q in range(chunks):
                    row = jnp.where(chunk == q, picked[g, h, q, pl.ds(a, 8, stride=8), :], row)
                rows.append(row)
            p = [
                jnp.where(good, got[d, a, r0 : r0 + 8, span], 0.0) for a in range(3)
            ]
            q = rows[:3]
            n = [jnp.where(good, row, 0.0) for row in rows[3:]]
            mis = n[0] * (p[0] - q[0]) + n[1] * (p[1] - q[1]) + n[2] * (p[2] - q[2])
            halves.append((cross(p, n) + n, cross(q, n) + n, mis))
        own_row = jnp.zeros((8, LANES), jnp.float32)
        far_row = jnp.zeros((8, LANES), jnp.float32)

        def total(make):
            acc = None
            for half in halves:
                acc = make(half) if acc is None else acc + make(half)
            return jnp.sum(acc, axis=1, keepdims=True)

        for f, (a, b) in enumerate(upper(6)):
            s = total(lambda v: v[0][a] * v[0][b])
            own_row = jnp.where(lane == PAIR * g + f, s, own_row)
            if a < 3:
                s = total(lambda v: v[1][a] * v[1][b])
            far_row = jnp.where(lane == f, s, far_row)
        for a in range(6):
            s = total(lambda v: v[0][a] * v[2])
            own_row = jnp.where(lane == PAIR * g + 21 + a, s, own_row)
            if a < 3:
                s = total(lambda v: v[1][a] * v[2])
            far_row = jnp.where(lane == 21 + a, -s, far_row)
        far[far_to, r0 : r0 + 8, :] = far_row
        return own_row

    def scatter(t, far_at):
        tot[...] += pick(scan == got_ids[t][:, :cap], far[far_at])

    far[1] = jnp.zeros(far.shape[1:], jnp.float32)

    def work(t, j):
        @pl.when(j > 0)
        def _():
            pts_copy(t, t).wait_recv()

        scatter(recv_at(jnp.maximum(j - 1, 0), me, tiles), (j + 1) % 2)
        for g in range(cap // 8):
            gather(t, g)

        @pl.when(j >= 0)
        def _():
            row = group(t, 0, j % 2)
            for g in range(1, cap // 8):
                row = row + group(t, g, j % 2)
            own[t] = row[:4] + pltpu.roll(row, LANES // 2, 1)[4:]

        @pl.when(j == 0)
        def _():
            back[grp * tiles + me] = own[t]

        @pl.when(j > 0)
        def _():
            own_copy(t, grp).start()

        own_copy(t, other).start()

    each(0, tiles, work, recv_at)
    scatter(recv_at(tiles - 1, me, tiles), (tiles - 1) % 2)
    seg_copy.wait_recv()
    all_of(pts, got, ps, pr.at[me], tiles - 1).wait_send()
    all_of(ids, got_ids, js, jr, tiles - 1).wait_send()
    seg_copy.wait_send()
    swap.start()
    all_of(back, back, ss, rs, 2 * tiles - 1).wait_recv()
    sums = tot[...]
    wide = lax.broadcasted_iota(jnp.int32, (SCANS_DEV, tiles * 4), 0)
    for mine, at in ((seg, grp), (seg_other, other)):
        rows = back[pl.ds(at * tiles, tiles)].reshape(tiles * 4, LANES)
        for g in range(cap // 8):
            for h in range(2):
                part = pick(wide == mine[2 * g + h : 2 * g + h + 1, :], rows)
                if g + h > 0:
                    part = pltpu.roll(part, LANES - PAIR * g - LANES // 2 * h, 1)
                sums = sums + part
    all_of(back, back, ss, rs, 2 * tiles - 1).wait_send()
    swap.wait()
    full = jnp.transpose(sums + partner[...])
    for a, row in enumerate(solve_rows([full[f : f + 1, :] for f in range(27)])):
        out[a : a + 1, :] = row


def solve_rows(rows):
    entries = {}
    for f, (a, b) in enumerate(upper(6)):
        entries[a, b] = rows[f]
    traced = entries[0, 0]
    for a in range(1, 6):
        traced = traced + entries[a, a]
    shift_by = DAMPING * traced / 6.0
    for a in range(6):
        entries[a, a] = entries[a, a] + shift_by
    values = [-rows[21 + a] for a in range(6)]
    for k in range(6):
        for a in range(k + 1, 6):
            factor = entries[k, a] / entries[k, k]
            for b in range(a, 6):
                entries[a, b] = entries[a, b] - factor * entries[k, b]
            values[a] = values[a] - factor * values[k]
    result = [None] * 6
    for a in range(5, -1, -1):
        running = values[a]
        for b in range(a + 1, 6):
            running = running - entries[a, b] * result[b]
        result[a] = running / entries[a, a]
    return result


def body(source_points, intersection, target_scan, matches, target_points, target_normals):
    tiles = lax.axis_size("tile")
    blocks = intersection.shape[1]
    points = source_points.shape[2] // blocks
    cap = -(-(2 * blocks // tiles) // 8) * 8
    f32, i32 = jnp.float32, jnp.int32
    shape = jax.ShapeDtypeStruct
    pts_t = (tiles, 4, cap, points)
    rows = (3, blocks * points // LANES, 1, LANES)
    ids_t, sums_t = (tiles, 1, LANES), (SCANS_DEV, LANES)
    return pl.pallas_call(
        main_kernel,
        out_shape=shape((6, SCANS_DEV), f32),
        in_specs=[ANY] * 6,
        out_specs=VMEM,
        scratch_shapes=[
            pltpu.VMEM((1, blocks), i32),
            pltpu.VMEM((1, blocks), i32),
            pltpu.VMEM(rows, f32),
            pltpu.VMEM(rows[1:], i32),
            pltpu.VMEM(target_points.shape, f32),
            pltpu.VMEM(target_normals.shape, f32),
            pltpu.VMEM((cap // 8, tiles * 8), i32),
            pltpu.SMEM((cap // 8, tiles * 8), i32),
            pltpu.VMEM(ids_t, i32),
            pltpu.VMEM((cap // 4, tiles * 4), i32),
            pltpu.VMEM((cap // 4, tiles * 4), i32),
            pltpu.VMEM(pts_t, f32),
            pltpu.VMEM(pts_t, f32),
            pltpu.VMEM(ids_t, i32),
            pltpu.SMEM(ids_t, i32),
            pltpu.VMEM((SCANS_DEV, 8, TARGET_PTS - LANES), f32),
            pltpu.VMEM((cap // 8, points // LANES, TARGET_PTS // LANES - 1, 64, LANES), f32),
            pltpu.VMEM((tiles, 4, LANES), f32),
            pltpu.VMEM((2, cap, LANES), f32),
            pltpu.VMEM((2 * tiles, 4, LANES), f32),
            pltpu.VMEM(sums_t, f32),
            pltpu.VMEM(sums_t, f32),
        ]
        + [pltpu.SemaphoreType.DMA((tiles,))]
        + [pltpu.SemaphoreType.DMA] * 5
        + [pltpu.SemaphoreType.DMA((9,))]
        + [pltpu.SemaphoreType.DMA] * 4,
        compiler_params=pltpu.CompilerParams(collective_id=0, has_side_effects=True),
        name="main",
    )(
        intersection.reshape(1, blocks),
        target_scan,
        source_points.reshape(rows),
        matches.reshape(rows[1:]),
        target_points,
        target_normals,
    )


def solution(mesh):
    in_specs = (
        P("grp", None, "tile"),
        P("grp", "tile", None),
        P("grp", "tile"),
        P("grp", "tile"),
        P(None, "tile"),
        P(None, "tile"),
    )
    out_specs = P(None, "tile")
    return jax.shard_map(body, mesh=mesh, in_specs=in_specs, out_specs=out_specs, check_vma=False)
```

```python
import jax
import jax.numpy as jnp
from jax import lax
from jax.experimental import pallas as pl
from jax.experimental.pallas import tpu as pltpu
from jax.sharding import PartitionSpec as P

SCANS_DEV = 64
TARGET_PTS = 512
DAMPING = 0.1
LANES = 128
PAIR = 32
AHEAD = 3
MESH = pl.DeviceIdType.MESH
VMEM = pl.BlockSpec(memory_space=pltpu.VMEM)
ANY = pl.BlockSpec(memory_space=pl.ANY)


def spread(to, rows, wide):
    for g in range(to.shape[0]):
        to[g : g + 1, :] = jnp.concatenate(
            [rows[t : t + 1, g * wide : (g + 1) * wide] for t in range(rows.shape[0])], axis=1
        )


def plan(dest, chosen, block, ids, seg):
    tiles = ids.shape[0]
    blocks = dest.shape[1]
    cap = seg.shape[0] * 4
    per_scan = blocks // SCANS_DEV
    f32 = jnp.float32
    hit = dest[...] == lax.broadcasted_iota(jnp.int32, (tiles, blocks), 0)
    first = lax.broadcasted_iota(jnp.int32, (blocks, blocks), 0)
    second = lax.broadcasted_iota(jnp.int32, (blocks, blocks), 1)
    rank = jnp.dot(
        hit.astype(f32), (first <= second).astype(f32), preferred_element_type=f32
    ).astype(jnp.int32)
    rank = jnp.where(hit, rank, 0)
    place = lax.broadcasted_iota(jnp.int32, (tiles, blocks), 1).astype(f32) + 1.0
    wanted = chosen[...].astype(f32) + 1.0
    lane = lax.broadcasted_iota(jnp.int32, (tiles, LANES), 1)
    at = jnp.zeros((tiles, LANES), f32)
    named = jnp.zeros((tiles, LANES), f32)
    for r in range(cap):
        mine = rank == r + 1
        at = jnp.where(
            lane == r, jnp.sum(jnp.where(mine, place, 0.0), axis=1, keepdims=True), at
        )
        named = jnp.where(
            lane == r, jnp.sum(jnp.where(mine, wanted, 0.0), axis=1, keepdims=True), named
        )
    at = at.astype(jnp.int32) - 1
    named = named.astype(jnp.int32) - 1
    spread(block, at, 8)
    scan = jnp.where(at >= 0, at // per_scan, -1)
    for t in range(tiles):
        ids[t] = named[t : t + 1]
    spread(seg, scan, 4)


def flip(me, k, tiles):
    other, bit = 0, 1
    while bit < tiles:
        other = other + (me // bit + k // bit) % 2 * bit
        bit *= 2
    return other


def send_at(j, me, tiles):
    half, quarter = tiles // 2, tiles // 4
    i = j // 2
    place = me // quarter
    inner = (place // 2 + place) % 2
    code = 3 - (inner * (1 - i // quarter) + (1 - inner) * (i % 2))
    low = inner * (i % quarter) + (1 - inner) * (i // 2)
    far = code * quarter + quarter - 1 - low
    return flip(me, jnp.where(j % 2 == 1, far, half - i), tiles)


def recv_at(j, me, tiles):
    half, quarter = tiles // 2, tiles // 4
    place = me // quarter
    inner = (place // 2 + place) % 2
    last = j // (tiles - 1)
    i = j // 2 - 1 + last
    second = i // quarter
    code = 3 - (inner + second) % 2
    far = code * quarter + quarter - 1 - i % quarter
    near = (half - (j + 1) // 2) * jnp.minimum(j, 1)
    return flip(me, jnp.where((j > 0) & (j % 2 - last == 0), far, near), tiles)


def pick(here, rows):
    bf16, f32 = jnp.bfloat16, jnp.float32
    parts = []
    for _ in range(3):
        parts.append(rows.astype(bf16))
        rows = rows - parts[-1].astype(f32)
    here = here.astype(f32).astype(bf16)
    return jnp.dot(
        jnp.concatenate([here] * 3, axis=1),
        jnp.concatenate(parts, axis=0),
        preferred_element_type=f32,
    )


def cross(u, v):
    return [
        u[1] * v[2] - u[2] * v[1],
        u[2] * v[0] - u[0] * v[2],
        u[0] * v[1] - u[1] * v[0],
    ]


def upper(vec):
    return [(a, b) for a in range(6) for b in range(a, 6)]


def main_kernel(
    dest_in, chosen_in, sp_in, mt_in, tp_in, tn_in, out,
    dest, chosen, sp, mt, tp, tn, places, block, ids, seg,
    seg_other, pts, got, got_ids, named, table, picked, own, far, back, tot, partner,
    pr, ps, js, jr, ss, rs, ls, hs, hr, gs, gr,
):
    tiles, _, cap, points = pts.shape
    blocks = dest.shape[1]
    me = lax.axis_index("tile")
    grp = lax.axis_index("grp")
    other = 1 - grp
    barrier = pltpu.get_barrier_semaphore()

    def greet(k, c):
        to = lax.rem(me + k, tiles)
        for side in range(2):
            pl.semaphore_signal(
                barrier, inc=1, device_id={"grp": side, "tile": to}, device_id_type=MESH
            )
        return c

    pl.semaphore_signal(barrier, inc=1, device_id={"grp": other}, device_id_type=MESH)
    lax.fori_loop(1, tiles, greet, 0)
    loads = [
        pltpu.make_async_copy(src, dst, ls.at[i])
        for i, (src, dst) in enumerate(
            [(dest_in, dest), (chosen_in, chosen), (sp_in, sp), (mt_in, mt), (tp_in, tp), (tn_in, tn)]
        )
    ]
    for load in loads:
        load.start()

    def remote(src, dst, send, recv, to, side=grp):
        return pltpu.make_async_remote_copy(
            src, dst, send, recv, {"grp": side, "tile": to}, MESH
        )

    def id_copy(t):
        return remote(ids.at[t], got_ids.at[me], js, jr, t)

    def pts_copy(to, frm):
        return remote(pts.at[to], got.at[frm], ps, pr.at[frm], to)

    def own_copy(t, side):
        return remote(own.at[t], back.at[grp * tiles + me], ss, rs, t, side)

    def all_of(src, dst, send, recv, count):
        span = pl.ds(0, count)
        return remote(src.at[span], dst.at[span], send, recv, me, other)

    seg_copy = remote(seg, seg_other, hs, hr, me, other)
    swap = remote(tot, partner, gs, gr, me, other)

    def each(start, stop, act, at=send_at):
        def one(j, c):
            act(at(j, me, tiles), j)
            return c

        lax.fori_loop(start, stop, one, 0)

    def pack(t, to, at_to):
        for r in range(cap):
            b = block[r // 8, t * 8 + r % 8]
            used = jnp.minimum(b, 0) + 1
            for h in range(points // LANES):
                span = slice(h * LANES, (h + 1) * LANES)
                at = jnp.clip(b, 0, blocks - 1) * (points // LANES) + h
                for a in range(3):
                    to[at_to, a, r : r + 1, span] = sp[a, at]
                to[at_to, 3, r : r + 1, span] = (mt[at] * used + (used - 1)).astype(jnp.float32)

    loads[0].wait()
    loads[1].wait()
    plan(dest, chosen, places, ids, seg)
    to_smem = pltpu.make_async_copy(places, block, ls.at[6])
    to_smem.start()
    loads[2].wait()
    loads[3].wait()
    to_smem.wait()
    ahead = min(AHEAD, tiles - 1)
    each(1, ahead + 1, lambda t, j: pack(t, pts, t))
    pl.semaphore_wait(barrier, 2 * tiles - 1)
    each(1, tiles, lambda t, j: id_copy(t).start())
    each(1, ahead + 1, lambda t, j: pts_copy(t, me).start())
    seg_copy.start()

    def pack_send(t, j):
        @pl.when(j < tiles)
        def _():
            pack(t, pts, t)

        @pl.when(j > ahead + 1)
        def _():
            pts_copy(send_at(j - 1, me, tiles), me).start()

    each(ahead + 1, tiles + 1, pack_send)
    self_ids = pltpu.make_async_copy(ids.at[me], got_ids.at[me], ls.at[7])
    self_ids.start()
    pack(me, got, me)
    loads[4].wait()
    loads[5].wait()

    chunks = TARGET_PTS // LANES - 1

    def fill(s, c):
        def cols(q):
            return pl.ds(pl.multiple_of(s * TARGET_PTS + q * LANES, LANES), LANES)

        for q in range(chunks):
            span = slice(q * LANES, (q + 1) * LANES)
            table[s, 0:3, span] = tp[:, cols(q)]
            table[s, 3:6, span] = tn[:, cols(q)]
            for r in range(2):
                ref, a = ((tp, 2 * q + r), (tn, 2 * q + r - 3))[2 * q + r > 2]
                table[s, 6 + r : 7 + r, span] = ref[a : a + 1, cols(chunks)]
        return c

    lax.fori_loop(0, SCANS_DEV, fill, 0, unroll=4)
    tot[...] = jnp.zeros(tot.shape, jnp.float32)
    self_ids.wait()
    all_of(ids, got_ids, js, jr, tiles - 1).wait_recv()
    load_ids = pltpu.make_async_copy(got_ids, named, ls.at[8])
    load_ids.start()
    load_ids.wait()
    lane = lax.broadcasted_iota(jnp.int32, (8, LANES), 1)
    scan = lax.broadcasted_iota(jnp.int32, (SCANS_DEV, cap), 0)
    halves_of = points // LANES

    def gather(d, g):
        r0 = g * 8
        near = got[d, 3, r0 : r0 + 8, :].astype(jnp.int32)
        for j in range(8):
            tab = table.at[jnp.clip(named[d, 0, r0 + j], 0, SCANS_DEV - 1)]
            for h in range(halves_of):
                at = jnp.broadcast_to(near[j : j + 1, h * LANES : (h + 1) * LANES], (8, LANES))
                low = at & (LANES - 1)
                for q in range(chunks):
                    picked[g, h, q, j * 8 : j * 8 + 8, :] = jnp.take_along_axis(
                        tab[:, q * LANES : (q + 1) * LANES],
                        low,
                        axis=1,
                        mode="promise_in_bounds",
                    )

    def group(d, g, far_to):
        r0 = g * 8
        near = got[d, 3, r0 : r0 + 8, :].astype(jnp.int32)
        halves = []
        for h in range(halves_of):
            span = slice(h * LANES, (h + 1) * LANES)
            good = near[:, span] >= 0
            chunk = (near[:, span] >> 7) & chunks
            rows = []
            for a in range(6):
                row = picked[g, h, a // 2, pl.ds(6 + a % 2, 8, stride=8), :]
                for q in range(chunks):
                    row = jnp.where(chunk == q, picked[g, h, q, pl.ds(a, 8, stride=8), :], row)
                rows.append(row)
            p = [
                jnp.where(good, got[d, a, r0 : r0 + 8, span], 0.0) for a in range(3)
            ]
            q = rows[:3]
            n = [jnp.where(good, row, 0.0) for row in rows[3:]]
            mis = n[0] * (p[0] - q[0]) + n[1] * (p[1] - q[1]) + n[2] * (p[2] - q[2])
            halves.append((cross(p, n) + n, cross(q, n) + n, mis))
        own_row = jnp.zeros((8, LANES), jnp.float32)
        far_row = jnp.zeros((8, LANES), jnp.float32)

        def total(make):
            acc = None
            for half in halves:
                acc = make(half) if acc is None else acc + make(half)
            return jnp.sum(acc, axis=1, keepdims=True)

        for f, (a, b) in enumerate(upper(6)):
            s = total(lambda v: v[0][a] * v[0][b])
            own_row = jnp.where(lane == PAIR * g + f, s, own_row)
            if a < 3:
                s = total(lambda v: v[1][a] * v[1][b])
            far_row = jnp.where(lane == f, s, far_row)
        for a in range(6):
            s = total(lambda v: v[0][a] * v[2])
            own_row = jnp.where(lane == PAIR * g + 21 + a, s, own_row)
            if a < 3:
                s = total(lambda v: v[1][a] * v[2])
            far_row = jnp.where(lane == 21 + a, -s, far_row)
        far[far_to, r0 : r0 + 8, :] = far_row
        return own_row

    def scatter(t, far_at):
        tot[...] += pick(scan == got_ids[t][:, :cap], far[far_at])

    far[1] = jnp.zeros(far.shape[1:], jnp.float32)

    def work(t, j):
        @pl.when(j > 0)
        def _():
            pts_copy(t, t).wait_recv()

        scatter(recv_at(jnp.maximum(j - 1, 0), me, tiles), (j + 1) % 2)
        for g in range(cap // 8):
            gather(t, g)

        @pl.when(j >= 0)
        def _():
            row = group(t, 0, j % 2)
            for g in range(1, cap // 8):
                row = row + group(t, g, j % 2)
            own[t] = row[:4] + pltpu.roll(row, LANES // 2, 1)[4:]

        @pl.when(j == 0)
        def _():
            back[grp * tiles + me] = own[t]

        @pl.when(j > 0)
        def _():
            own_copy(t, grp).start()

        own_copy(t, other).start()

    each(0, tiles, work, recv_at)
    scatter(recv_at(tiles - 1, me, tiles), (tiles - 1) % 2)
    seg_copy.wait_recv()
    all_of(pts, got, ps, pr.at[me], tiles - 1).wait_send()
    all_of(ids, got_ids, js, jr, tiles - 1).wait_send()
    seg_copy.wait_send()
    swap.start()
    all_of(back, back, ss, rs, 2 * tiles - 1).wait_recv()
    sums = tot[...]
    wide = lax.broadcasted_iota(jnp.int32, (SCANS_DEV, tiles * 4), 0)
    for mine, at in ((seg, grp), (seg_other, other)):
        rows = back[pl.ds(at * tiles, tiles)].reshape(tiles * 4, LANES)
        for g in range(cap // 8):
            for h in range(2):
                part = pick(wide == mine[2 * g + h : 2 * g + h + 1, :], rows)
                if g + h > 0:
                    part = pltpu.roll(part, LANES - PAIR * g - LANES // 2 * h, 1)
                sums = sums + part
    all_of(back, back, ss, rs, 2 * tiles - 1).wait_send()
    swap.wait()
    full = jnp.transpose(sums + partner[...])
    for a, row in enumerate(solve_rows([full[f : f + 1, :] for f in range(27)])):
        out[a : a + 1, :] = row


def solve_rows(rows):
    entries = {}
    for f, (a, b) in enumerate(upper(6)):
        entries[a, b] = rows[f]
    traced = entries[0, 0]
    for a in range(1, 6):
        traced = traced + entries[a, a]
    shift_by = DAMPING * traced / 6.0
    for a in range(6):
        entries[a, a] = entries[a, a] + shift_by
    values = [-rows[21 + a] for a in range(6)]
    for k in range(6):
        for a in range(k + 1, 6):
            factor = entries[k, a] / entries[k, k]
            for b in range(a, 6):
                entries[a, b] = entries[a, b] - factor * entries[k, b]
            values[a] = values[a] - factor * values[k]
    result = [None] * 6
    for a in range(5, -1, -1):
        running = values[a]
        for b in range(a + 1, 6):
            running = running - entries[a, b] * result[b]
        result[a] = running / entries[a, a]
    return result


def body(source_points, intersection, target_scan, matches, target_points, target_normals):
    tiles = lax.axis_size("tile")
    blocks = intersection.shape[1]
    points = source_points.shape[2] // blocks
    cap = -(-(2 * blocks // tiles) // 8) * 8
    f32, i32 = jnp.float32, jnp.int32
    shape = jax.ShapeDtypeStruct
    pts_t = (tiles, 4, cap, points)
    rows = (3, blocks * points // LANES, 1, LANES)
    ids_t, sums_t = (tiles, 1, LANES), (SCANS_DEV, LANES)
    return pl.pallas_call(
        main_kernel,
        out_shape=pltpu.VMEM((6, SCANS_DEV), f32),
        in_specs=[ANY] * 6,
        out_specs=VMEM,
        scratch_shapes=[
            pltpu.VMEM((1, blocks), i32),
            pltpu.VMEM((1, blocks), i32),
            pltpu.VMEM(rows, f32),
            pltpu.VMEM(rows[1:], i32),
            pltpu.VMEM(target_points.shape, f32),
            pltpu.VMEM(target_normals.shape, f32),
            pltpu.VMEM((cap // 8, tiles * 8), i32),
            pltpu.SMEM((cap // 8, tiles * 8), i32),
            pltpu.VMEM(ids_t, i32),
            pltpu.VMEM((cap // 4, tiles * 4), i32),
            pltpu.VMEM((cap // 4, tiles * 4), i32),
            pltpu.VMEM(pts_t, f32),
            pltpu.VMEM(pts_t, f32),
            pltpu.VMEM(ids_t, i32),
            pltpu.SMEM(ids_t, i32),
            pltpu.VMEM((SCANS_DEV, 8, TARGET_PTS - LANES), f32),
            pltpu.VMEM((cap // 8, points // LANES, TARGET_PTS // LANES - 1, 64, LANES), f32),
            pltpu.VMEM((tiles, 4, LANES), f32),
            pltpu.VMEM((2, cap, LANES), f32),
            pltpu.VMEM((2 * tiles, 4, LANES), f32),
            pltpu.VMEM(sums_t, f32),
            pltpu.VMEM(sums_t, f32),
        ]
        + [pltpu.SemaphoreType.DMA((tiles,))]
        + [pltpu.SemaphoreType.DMA] * 5
        + [pltpu.SemaphoreType.DMA((9,))]
        + [pltpu.SemaphoreType.DMA] * 4,
        compiler_params=pltpu.CompilerParams(collective_id=0, has_side_effects=True),
        name="main",
    )(
        intersection.reshape(1, blocks),
        target_scan,
        source_points.reshape(rows),
        matches.reshape(rows[1:]),
        target_points,
        target_normals,
    )


def solution(mesh):
    in_specs = (
        P("grp", None, "tile"),
        P("grp", "tile", None),
        P("grp", "tile"),
        P("grp", "tile"),
        P(None, "tile"),
        P(None, "tile"),
    )
    out_specs = P(None, "tile")
    return jax.shard_map(body, mesh=mesh, in_specs=in_specs, out_specs=out_specs, check_vma=False)
```

```python
import jax
import jax.numpy as jnp
from jax import lax
from jax.experimental import pallas as pl
from jax.experimental.pallas import tpu as pltpu
from jax.sharding import PartitionSpec as P

SCANS_DEV = 64
TARGET_PTS = 512
DAMPING = 0.1
LANES = 128
PAIR = 32
AHEAD = 2
MESH = pl.DeviceIdType.MESH
VMEM = pl.BlockSpec(memory_space=pltpu.VMEM)
ANY = pl.BlockSpec(memory_space=pl.ANY)


def spread(to, rows, wide):
    for g in range(to.shape[0]):
        to[g : g + 1, :] = jnp.concatenate(
            [rows[t : t + 1, g * wide : (g + 1) * wide] for t in range(rows.shape[0])], axis=1
        )


def plan(dest, chosen, block, ids, seg, ready):
    tiles = ids.shape[0]
    blocks = dest.shape[1]
    cap = seg.shape[0] * 4
    per_scan = blocks // SCANS_DEV
    f32 = jnp.float32
    hit = dest[...] == lax.broadcasted_iota(jnp.int32, (tiles, blocks), 0)
    first = lax.broadcasted_iota(jnp.int32, (blocks, blocks), 0)
    second = lax.broadcasted_iota(jnp.int32, (blocks, blocks), 1)
    rank = jnp.dot(
        hit.astype(f32), (first <= second).astype(f32), preferred_element_type=f32
    ).astype(jnp.int32)
    rank = jnp.where(hit, rank, 0)
    lane = lax.broadcasted_iota(jnp.int32, (tiles, LANES), 1)

    def listed(values):
        out = jnp.zeros((tiles, LANES), f32)
        for r in range(cap):
            value = jnp.sum(jnp.where(rank == r + 1, values, 0.0), axis=1, keepdims=True)
            out = jnp.where(lane == r, value, out)
        return out.astype(jnp.int32) - 1

    place = lax.broadcasted_iota(jnp.int32, (tiles, blocks), 1).astype(f32) + 1.0
    at = listed(place)
    spread(block, at, 8)
    ready()
    named = listed(chosen[...].astype(f32) + 1.0)
    scan = jnp.where(at >= 0, at // per_scan, -1)
    for t in range(tiles):
        ids[t] = named[t : t + 1]
    spread(seg, scan, 4)


def flip(me, k, tiles):
    other, bit = 0, 1
    while bit < tiles:
        other = other + (me // bit + k // bit) % 2 * bit
        bit *= 2
    return other


def send_at(j, me, tiles):
    half, quarter = tiles // 2, tiles // 4
    i = jnp.where(j <= quarter, j - 1, jnp.where(j <= half + quarter, quarter + (j - quarter - 1) // 2, 0))
    n = jnp.where(j <= half + quarter, (j - quarter) // 2, j - half)
    place = me // quarter
    inner = (place // 2 + place) % 2
    code = 3 - (inner * (1 - i // quarter) + (1 - inner) * (i % 2))
    low = inner * (i % quarter) + (1 - inner) * (i // 2)
    far = code * quarter + quarter - 1 - low
    return flip(me, jnp.where((j <= quarter) | ((j <= half + quarter) & ((j - quarter) % 2 == 1)), far, half - n), tiles)


def recv_at(j, me, tiles):
    half, quarter = tiles // 2, tiles // 4
    place = me // quarter
    inner = (place // 2 + place) % 2
    last = j // (tiles - 1)
    i = j // 2 - 1 + last
    second = i // quarter
    code = 3 - (inner + second) % 2
    far = code * quarter + quarter - 1 - i % quarter
    near = (half - (j + 1) // 2) * jnp.minimum(j, 1)
    return flip(me, jnp.where((j > 0) & (j % 2 - last == 0), far, near), tiles)


def pick(here, rows):
    bf16, f32 = jnp.bfloat16, jnp.float32
    parts = []
    for _ in range(3):
        parts.append(rows.astype(bf16))
        rows = rows - parts[-1].astype(f32)
    here = here.astype(f32).astype(bf16)
    return jnp.dot(
        jnp.concatenate([here] * 3, axis=1),
        jnp.concatenate(parts, axis=0),
        preferred_element_type=f32,
    )


def cross(u, v):
    return [
        u[1] * v[2] - u[2] * v[1],
        u[2] * v[0] - u[0] * v[2],
        u[0] * v[1] - u[1] * v[0],
    ]


def upper(vec):
    return [(a, b) for a in range(6) for b in range(a, 6)]


def main_kernel(
    dest_in, chosen_in, sp_in, mt_in, tp_in, tn_in, out,
    dest, chosen, sp, mt, tp, tn, places, block, ids, seg,
    seg_other, pts, got, got_ids, named, table, picked, own, far, back, tot, partner,
    pr, ps, js, jr, ss, rs, ls, hs, hr, gs, gr,
):
    tiles, _, cap, points = pts.shape
    blocks = dest.shape[1]
    me = lax.axis_index("tile")
    grp = lax.axis_index("grp")
    other = 1 - grp
    barrier = pltpu.get_barrier_semaphore()

    def greet(k, c):
        to = lax.rem(me + k, tiles)
        for side in range(2):
            pl.semaphore_signal(
                barrier, inc=1, device_id={"grp": side, "tile": to}, device_id_type=MESH
            )
        return c

    pl.semaphore_signal(barrier, inc=1, device_id={"grp": other}, device_id_type=MESH)
    lax.fori_loop(1, tiles, greet, 0)
    loads = [
        pltpu.make_async_copy(src, dst, ls.at[i])
        for i, (src, dst) in enumerate(
            [(dest_in, dest), (chosen_in, chosen), (sp_in, sp), (mt_in, mt), (tp_in, tp), (tn_in, tn)]
        )
    ]
    for load in loads:
        load.start()

    def remote(src, dst, send, recv, to, side=grp):
        return pltpu.make_async_remote_copy(
            src, dst, send, recv, {"grp": side, "tile": to}, MESH
        )

    def id_copy(t):
        return remote(ids.at[t], got_ids.at[me], js, jr, t)

    def pts_copy(to, frm):
        return remote(pts.at[to], got.at[frm], ps, pr.at[frm], to)

    def own_copy(t, side):
        return remote(own.at[t], back.at[grp * tiles + me], ss, rs, t, side)

    def all_of(src, dst, send, recv, count):
        span = pl.ds(0, count)
        return remote(src.at[span], dst.at[span], send, recv, me, other)

    seg_copy = remote(seg, seg_other, hs, hr, me, other)
    swap = remote(tot, partner, gs, gr, me, other)

    def each(start, stop, act, at=send_at):
        def one(j, c):
            act(at(j, me, tiles), j)
            return c

        lax.fori_loop(start, stop, one, 0)

    def pack(t, to, at_to):
        for r in range(cap):
            b = block[r // 8, t * 8 + r % 8]
            used = jnp.minimum(b, 0) + 1
            for h in range(points // LANES):
                span = slice(h * LANES, (h + 1) * LANES)
                at = jnp.clip(b, 0, blocks - 1) * (points // LANES) + h
                for a in range(3):
                    to[at_to, a, r : r + 1, span] = sp[a, at]
                to[at_to, 3, r : r + 1, span] = (mt[at] * used + (used - 1)).astype(jnp.float32)

    loads[0].wait()
    loads[1].wait()
    to_smem = pltpu.make_async_copy(places, block, ls.at[6])
    plan(dest, chosen, places, ids, seg, to_smem.start)
    loads[2].wait()
    loads[3].wait()
    to_smem.wait()
    ahead = min(AHEAD, tiles - 1)
    each(1, ahead + 1, lambda t, j: pack(t, pts, t))
    pl.semaphore_wait(barrier, 2 * tiles - 1)
    each(1, tiles, lambda t, j: id_copy(t).start())
    each(1, ahead + 1, lambda t, j: pts_copy(t, me).start())
    seg_copy.start()

    def pack_send(t, j):
        @pl.when(j < tiles)
        def _():
            pack(t, pts, t)

        @pl.when(j > ahead + 1)
        def _():
            pts_copy(send_at(j - 1, me, tiles), me).start()

    each(ahead + 1, tiles + 1, pack_send)
    self_ids = pltpu.make_async_copy(ids.at[me], got_ids.at[me], ls.at[7])
    self_ids.start()
    pack(me, got, me)
    loads[4].wait()
    loads[5].wait()

    chunks = TARGET_PTS // LANES - 1

    def fill(s, c):
        def cols(q):
            return pl.ds(pl.multiple_of(s * TARGET_PTS + q * LANES, LANES), LANES)

        for q in range(chunks):
            span = slice(q * LANES, (q + 1) * LANES)
            table[s, 0:3, span] = tp[:, cols(q)]
            table[s, 3:6, span] = tn[:, cols(q)]
            for r in range(2):
                ref, a = ((tp, 2 * q + r), (tn, 2 * q + r - 3))[2 * q + r > 2]
                table[s, 6 + r : 7 + r, span] = ref[a : a + 1, cols(chunks)]
        return c

    lax.fori_loop(0, SCANS_DEV, fill, 0, unroll=4)
    tot[...] = jnp.zeros(tot.shape, jnp.float32)
    self_ids.wait()
    all_of(ids, got_ids, js, jr, tiles - 1).wait_recv()
    load_ids = pltpu.make_async_copy(got_ids, named, ls.at[8])
    load_ids.start()
    load_ids.wait()
    lane = lax.broadcasted_iota(jnp.int32, (8, LANES), 1)
    scan = lax.broadcasted_iota(jnp.int32, (SCANS_DEV, cap), 0)
    halves_of = points // LANES

    def gather(d, g):
        r0 = g * 8
        near = got[d, 3, r0 : r0 + 8, :].astype(jnp.int32)
        for j in range(8):
            tab = table.at[jnp.clip(named[d, 0, r0 + j], 0, SCANS_DEV - 1)]
            for h in range(halves_of):
                at = jnp.broadcast_to(near[j : j + 1, h * LANES : (h + 1) * LANES], (8, LANES))
                low = at & (LANES - 1)
                for q in range(chunks):
                    picked[g, h, q, j * 8 : j * 8 + 8, :] = jnp.take_along_axis(
                        tab[:, q * LANES : (q + 1) * LANES],
                        low,
                        axis=1,
                        mode="promise_in_bounds",
                    )

    def group(d, g, far_to):
        r0 = g * 8
        near = got[d, 3, r0 : r0 + 8, :].astype(jnp.int32)
        halves = []
        for h in range(halves_of):
            span = slice(h * LANES, (h + 1) * LANES)
            good = near[:, span] >= 0
            chunk = (near[:, span] >> 7) & chunks
            rows = []
            for a in range(6):
                row = picked[g, h, a // 2, pl.ds(6 + a % 2, 8, stride=8), :]
                for q in range(chunks):
                    row = jnp.where(chunk == q, picked[g, h, q, pl.ds(a, 8, stride=8), :], row)
                rows.append(row)
            p = [
                jnp.where(good, got[d, a, r0 : r0 + 8, span], 0.0) for a in range(3)
            ]
            q = rows[:3]
            n = [jnp.where(good, row, 0.0) for row in rows[3:]]
            mis = n[0] * (p[0] - q[0]) + n[1] * (p[1] - q[1]) + n[2] * (p[2] - q[2])
            halves.append((cross(p, n) + n, cross(q, n) + n, mis))
        own_row = jnp.zeros((8, LANES), jnp.float32)
        far_row = jnp.zeros((8, LANES), jnp.float32)

        def total(make):
            acc = None
            for half in halves:
                acc = make(half) if acc is None else acc + make(half)
            return jnp.sum(acc, axis=1, keepdims=True)

        for f, (a, b) in enumerate(upper(6)):
            s = total(lambda v: v[0][a] * v[0][b])
            own_row = jnp.where(lane == PAIR * g + f, s, own_row)
            if a < 3:
                s = total(lambda v: v[1][a] * v[1][b])
            far_row = jnp.where(lane == f, s, far_row)
        for a in range(6):
            s = total(lambda v: v[0][a] * v[2])
            own_row = jnp.where(lane == PAIR * g + 21 + a, s, own_row)
            if a < 3:
                s = total(lambda v: v[1][a] * v[2])
            far_row = jnp.where(lane == 21 + a, -s, far_row)
        far[far_to, r0 : r0 + 8, :] = far_row
        return own_row

    def scatter(t, far_at):
        tot[...] += pick(scan == got_ids[t][:, :cap], far[far_at])

    far[1] = jnp.zeros(far.shape[1:], jnp.float32)

    def work(t, j):
        @pl.when(j > 0)
        def _():
            pts_copy(t, t).wait_recv()

        scatter(recv_at(jnp.maximum(j - 1, 0), me, tiles), (j + 1) % 2)
        for g in range(cap // 8):
            gather(t, g)

        @pl.when(j >= 0)
        def _():
            row = group(t, 0, j % 2)
            for g in range(1, cap // 8):
                row = row + group(t, g, j % 2)
            own[t] = row[:4] + pltpu.roll(row, LANES // 2, 1)[4:]

        @pl.when(j == 0)
        def _():
            back[grp * tiles + me] = own[t]

        @pl.when(j > 0)
        def _():
            own_copy(t, grp).start()

        own_copy(t, other).start()

    each(0, tiles, work, recv_at)
    scatter(recv_at(tiles - 1, me, tiles), (tiles - 1) % 2)
    seg_copy.wait_recv()
    all_of(pts, got, ps, pr.at[me], tiles - 1).wait_send()
    all_of(ids, got_ids, js, jr, tiles - 1).wait_send()
    seg_copy.wait_send()
    swap.start()
    all_of(back, back, ss, rs, 2 * tiles - 1).wait_recv()
    sums = tot[...]
    wide = lax.broadcasted_iota(jnp.int32, (SCANS_DEV, tiles * 4), 0)
    for mine, at in ((seg, grp), (seg_other, other)):
        rows = back[pl.ds(at * tiles, tiles)].reshape(tiles * 4, LANES)
        for g in range(cap // 8):
            for h in range(2):
                part = pick(wide == mine[2 * g + h : 2 * g + h + 1, :], rows)
                if g + h > 0:
                    part = pltpu.roll(part, LANES - PAIR * g - LANES // 2 * h, 1)
                sums = sums + part
    all_of(back, back, ss, rs, 2 * tiles - 1).wait_send()
    swap.wait()
    full = jnp.transpose(sums + partner[...])
    for a, row in enumerate(solve_rows([full[f : f + 1, :] for f in range(27)])):
        out[a : a + 1, :] = row


def solve_rows(rows):
    entries = {}
    for f, (a, b) in enumerate(upper(6)):
        entries[a, b] = rows[f]
    traced = entries[0, 0]
    for a in range(1, 6):
        traced = traced + entries[a, a]
    shift_by = DAMPING * traced / 6.0
    for a in range(6):
        entries[a, a] = entries[a, a] + shift_by
    values = [-rows[21 + a] for a in range(6)]
    for k in range(6):
        for a in range(k + 1, 6):
            factor = entries[k, a] / entries[k, k]
            for b in range(a, 6):
                entries[a, b] = entries[a, b] - factor * entries[k, b]
            values[a] = values[a] - factor * values[k]
    result = [None] * 6
    for a in range(5, -1, -1):
        running = values[a]
        for b in range(a + 1, 6):
            running = running - entries[a, b] * result[b]
        result[a] = running / entries[a, a]
    return result


def body(source_points, intersection, target_scan, matches, target_points, target_normals):
    tiles = lax.axis_size("tile")
    blocks = intersection.shape[1]
    points = source_points.shape[2] // blocks
    cap = -(-(2 * blocks // tiles) // 8) * 8
    f32, i32 = jnp.float32, jnp.int32
    shape = jax.ShapeDtypeStruct
    pts_t = (tiles, 4, cap, points)
    rows = (3, blocks * points // LANES, 1, LANES)
    ids_t, sums_t = (tiles, 1, LANES), (SCANS_DEV, LANES)
    return pl.pallas_call(
        main_kernel,
        out_shape=pltpu.VMEM((6, SCANS_DEV), f32),
        in_specs=[ANY] * 6,
        out_specs=VMEM,
        scratch_shapes=[
            pltpu.VMEM((1, blocks), i32),
            pltpu.VMEM((1, blocks), i32),
            pltpu.VMEM(rows, f32),
            pltpu.VMEM(rows[1:], i32),
            pltpu.VMEM(target_points.shape, f32),
            pltpu.VMEM(target_normals.shape, f32),
            pltpu.VMEM((cap // 8, tiles * 8), i32),
            pltpu.SMEM((cap // 8, tiles * 8), i32),
            pltpu.VMEM(ids_t, i32),
            pltpu.VMEM((cap // 4, tiles * 4), i32),
            pltpu.VMEM((cap // 4, tiles * 4), i32),
            pltpu.VMEM(pts_t, f32),
            pltpu.VMEM(pts_t, f32),
            pltpu.VMEM(ids_t, i32),
            pltpu.SMEM(ids_t, i32),
            pltpu.VMEM((SCANS_DEV, 8, TARGET_PTS - LANES), f32),
            pltpu.VMEM((cap // 8, points // LANES, TARGET_PTS // LANES - 1, 64, LANES), f32),
            pltpu.VMEM((tiles, 4, LANES), f32),
            pltpu.VMEM((2, cap, LANES), f32),
            pltpu.VMEM((2 * tiles, 4, LANES), f32),
            pltpu.VMEM(sums_t, f32),
            pltpu.VMEM(sums_t, f32),
        ]
        + [pltpu.SemaphoreType.DMA((tiles,))]
        + [pltpu.SemaphoreType.DMA] * 5
        + [pltpu.SemaphoreType.DMA((9,))]
        + [pltpu.SemaphoreType.DMA] * 4,
        compiler_params=pltpu.CompilerParams(collective_id=0, has_side_effects=True),
        name="main",
    )(
        intersection.reshape(1, blocks),
        target_scan,
        source_points.reshape(rows),
        matches.reshape(rows[1:]),
        target_points,
        target_normals,
    )


def solution(mesh):
    in_specs = (
        P("grp", None, "tile"),
        P("grp", "tile", None),
        P("grp", "tile"),
        P("grp", "tile"),
        P(None, "tile"),
        P(None, "tile"),
    )
    out_specs = P(None, "tile")
    return jax.shard_map(body, mesh=mesh, in_specs=in_specs, out_specs=out_specs, check_vma=False)
```

```python
import jax
import jax.numpy as jnp
from jax import lax
from jax.experimental import pallas as pl
from jax.experimental.pallas import tpu as pltpu
from jax.sharding import PartitionSpec as P

SCANS_DEV = 64
TARGET_PTS = 512
DAMPING = 0.1
LANES = 128
PAIR = 32
AHEAD = 2
MESH = pl.DeviceIdType.MESH
VMEM = pl.BlockSpec(memory_space=pltpu.VMEM)
ANY = pl.BlockSpec(memory_space=pl.ANY)


def spread(to, rows, wide):
    for g in range(to.shape[0]):
        to[g : g + 1, :] = jnp.concatenate(
            [rows[t : t + 1, g * wide : (g + 1) * wide] for t in range(rows.shape[0])], axis=1
        )


def plan(dest, chosen, block, ids, seg, ready):
    tiles = ids.shape[0]
    blocks = dest.shape[1]
    cap = seg.shape[0] * 4
    per_scan = blocks // SCANS_DEV
    f32 = jnp.float32
    hit = dest[...] == lax.broadcasted_iota(jnp.int32, (tiles, blocks), 0)
    first = lax.broadcasted_iota(jnp.int32, (blocks, blocks), 0)
    second = lax.broadcasted_iota(jnp.int32, (blocks, blocks), 1)
    rank = jnp.dot(
        hit.astype(f32), (first <= second).astype(f32), preferred_element_type=f32
    ).astype(jnp.int32)
    rank = jnp.where(hit, rank, 0)
    lane = lax.broadcasted_iota(jnp.int32, (tiles, LANES), 1)

    def listed(values):
        out = jnp.zeros((tiles, LANES), f32)
        for r in range(cap):
            value = jnp.sum(jnp.where(rank == r + 1, values, 0.0), axis=1, keepdims=True)
            out = jnp.where(lane == r, value, out)
        return out.astype(jnp.int32) - 1

    place = lax.broadcasted_iota(jnp.int32, (tiles, blocks), 1).astype(f32) + 1.0
    at = listed(place)
    spread(block, at, 8)
    ready()
    named = listed(chosen[...].astype(f32) + 1.0)
    scan = jnp.where(at >= 0, at // per_scan, -1)
    for t in range(tiles):
        ids[t] = named[t : t + 1]
    spread(seg, scan, 4)


def flip(me, k, tiles):
    other, bit = 0, 1
    while bit < tiles:
        other = other + (me // bit + k // bit) % 2 * bit
        bit *= 2
    return other


def send_at(j, me, tiles):
    half, quarter = tiles // 2, tiles // 4
    i = jnp.where(j <= quarter, j - 1, jnp.where(j <= half + quarter, quarter + (j - quarter - 1) // 2, 0))
    n = jnp.where(j <= half + quarter, (j - quarter) // 2, j - half)
    place = me // quarter
    inner = (place // 2 + place) % 2
    code = 3 - (inner * (1 - i // quarter) + (1 - inner) * (i % 2))
    low = inner * (i % quarter) + (1 - inner) * (i // 2)
    far = code * quarter + quarter - 1 - low
    return flip(me, jnp.where((j <= quarter) | ((j <= half + quarter) & ((j - quarter) % 2 == 1)), far, half - n), tiles)


def recv_at(j, me, tiles):
    half, quarter = tiles // 2, tiles // 4
    place = me // quarter
    inner = (place // 2 + place) % 2
    last = j // (tiles - 1)
    i = j // 2 - 1 + last
    second = i // quarter
    code = 3 - (inner + second) % 2
    far = code * quarter + quarter - 1 - i % quarter
    near = (half - (j + 1) // 2) * jnp.minimum(j, 1)
    return flip(me, jnp.where((j > 0) & (j % 2 - last == 0), far, near), tiles)


def pick(here, rows):
    bf16, f32 = jnp.bfloat16, jnp.float32
    return pick_by(here.astype(f32).astype(bf16), rows)


def pick_by(here, rows):
    bf16, f32 = jnp.bfloat16, jnp.float32
    parts = []
    for _ in range(3):
        parts.append(rows.astype(bf16))
        rows = rows - parts[-1].astype(f32)
    return jnp.dot(
        jnp.concatenate([here] * 3, axis=1),
        jnp.concatenate(parts, axis=0),
        preferred_element_type=f32,
    )


def cross(u, v):
    return [
        u[1] * v[2] - u[2] * v[1],
        u[2] * v[0] - u[0] * v[2],
        u[0] * v[1] - u[1] * v[0],
    ]


def upper(vec):
    return [(a, b) for a in range(6) for b in range(a, 6)]


def main_kernel(
    dest_in, chosen_in, sp_in, mt_in, tp_in, tn_in, out,
    dest, chosen, sp, mt, tp, tn, places, block, ids, seg,
    seg_other, pts, got, got_ids, named, table, picked, own, far, back, tot, partner, masks,
    pr, ps, js, jr, ss, rs, ls, hs, hr, gs, gr,
):
    tiles, _, cap, points = pts.shape
    blocks = dest.shape[1]
    me = lax.axis_index("tile")
    grp = lax.axis_index("grp")
    other = 1 - grp
    barrier = pltpu.get_barrier_semaphore()

    loads = [
        pltpu.make_async_copy(src, dst, ls.at[i])
        for i, (src, dst) in enumerate(
            [(dest_in, dest), (chosen_in, chosen), (sp_in, sp), (mt_in, mt), (tp_in, tp), (tn_in, tn)]
        )
    ]
    for load in loads[:4]:
        load.start()

    def greet(k, c):
        to = lax.rem(me + k, tiles)
        for side in range(2):
            pl.semaphore_signal(
                barrier, inc=1, device_id={"grp": side, "tile": to}, device_id_type=MESH
            )
        return c

    pl.semaphore_signal(barrier, inc=1, device_id={"grp": other}, device_id_type=MESH)
    lax.fori_loop(1, tiles, greet, 0)
    for load in loads[4:]:
        load.start()

    def remote(src, dst, send, recv, to, side=grp):
        return pltpu.make_async_remote_copy(
            src, dst, send, recv, {"grp": side, "tile": to}, MESH
        )

    def id_copy(t):
        return remote(ids.at[t], got_ids.at[me], js, jr, t)

    def pts_copy(to, frm):
        return remote(pts.at[to], got.at[frm], ps, pr.at[frm], to)

    def own_copy(t, side):
        return remote(own.at[t], back.at[grp * tiles + me], ss, rs, t, side)

    def all_of(src, dst, send, recv, count):
        span = pl.ds(0, count)
        return remote(src.at[span], dst.at[span], send, recv, me, other)

    seg_copy = remote(seg, seg_other, hs, hr, me, other)
    swap = remote(tot, partner, gs, gr, me, other)

    def each(start, stop, act, at=send_at):
        def one(j, c):
            act(at(j, me, tiles), j)
            return c

        lax.fori_loop(start, stop, one, 0)

    def pack(t, to, at_to):
        for r in range(cap):
            b = block[r // 8, t * 8 + r % 8]
            used = jnp.minimum(b, 0) + 1
            for h in range(points // LANES):
                span = slice(h * LANES, (h + 1) * LANES)
                at = jnp.clip(b, 0, blocks - 1) * (points // LANES) + h
                for a in range(3):
                    to[at_to, a, r : r + 1, span] = sp[a, at]
                to[at_to, 3, r : r + 1, span] = (mt[at] * used + (used - 1)).astype(jnp.float32)

    loads[0].wait()
    loads[1].wait()
    to_smem = pltpu.make_async_copy(places, block, ls.at[6])
    plan(dest, chosen, places, ids, seg, to_smem.start)
    loads[2].wait()
    loads[3].wait()
    to_smem.wait()
    ahead = min(AHEAD, tiles - 1)
    each(1, ahead + 1, lambda t, j: pack(t, pts, t))
    pl.semaphore_wait(barrier, 2 * tiles - 1)
    each(1, tiles, lambda t, j: id_copy(t).start())
    each(1, ahead + 1, lambda t, j: pts_copy(t, me).start())
    seg_copy.start()

    def pack_send(t, j):
        @pl.when(j < tiles)
        def _():
            pack(t, pts, t)

        @pl.when(j > ahead + 1)
        def _():
            pts_copy(send_at(j - 1, me, tiles), me).start()

    each(ahead + 1, tiles + 1, pack_send)
    self_ids = pltpu.make_async_copy(ids.at[me], got_ids.at[me], ls.at[7])
    self_ids.start()
    pack(me, got, me)
    loads[4].wait()
    loads[5].wait()

    chunks = TARGET_PTS // LANES - 1

    def fill(s, c):
        def cols(q):
            return pl.ds(pl.multiple_of(s * TARGET_PTS + q * LANES, LANES), LANES)

        for q in range(chunks):
            span = slice(q * LANES, (q + 1) * LANES)
            table[s, 0:3, span] = tp[:, cols(q)]
            table[s, 3:6, span] = tn[:, cols(q)]
            for r in range(2):
                ref, a = ((tp, 2 * q + r), (tn, 2 * q + r - 3))[2 * q + r > 2]
                table[s, 6 + r : 7 + r, span] = ref[a : a + 1, cols(chunks)]
        return c

    lax.fori_loop(0, SCANS_DEV, fill, 0, unroll=4)
    tot[...] = jnp.zeros(tot.shape, jnp.float32)
    self_ids.wait()
    all_of(ids, got_ids, js, jr, tiles - 1).wait_recv()
    load_ids = pltpu.make_async_copy(got_ids, named, ls.at[8])
    load_ids.start()
    load_ids.wait()
    lane = lax.broadcasted_iota(jnp.int32, (8, LANES), 1)
    scan = lax.broadcasted_iota(jnp.int32, (SCANS_DEV, cap), 0)
    halves_of = points // LANES

    def gather(d, g):
        r0 = g * 8
        near = got[d, 3, r0 : r0 + 8, :].astype(jnp.int32)
        for j in range(8):
            tab = table.at[jnp.clip(named[d, 0, r0 + j], 0, SCANS_DEV - 1)]
            for h in range(halves_of):
                at = jnp.broadcast_to(near[j : j + 1, h * LANES : (h + 1) * LANES], (8, LANES))
                low = at & (LANES - 1)
                for q in range(chunks):
                    picked[g, h, q, j * 8 : j * 8 + 8, :] = jnp.take_along_axis(
                        tab[:, q * LANES : (q + 1) * LANES],
                        low,
                        axis=1,
                        mode="promise_in_bounds",
                    )

    def group(d, g, far_to):
        r0 = g * 8
        near = got[d, 3, r0 : r0 + 8, :].astype(jnp.int32)
        halves = []
        for h in range(halves_of):
            span = slice(h * LANES, (h + 1) * LANES)
            good = near[:, span] >= 0
            chunk = (near[:, span] >> 7) & chunks
            rows = []
            for a in range(6):
                row = picked[g, h, a // 2, pl.ds(6 + a % 2, 8, stride=8), :]
                for q in range(chunks):
                    row = jnp.where(chunk == q, picked[g, h, q, pl.ds(a, 8, stride=8), :], row)
                rows.append(row)
            p = [
                jnp.where(good, got[d, a, r0 : r0 + 8, span], 0.0) for a in range(3)
            ]
            q = rows[:3]
            n = [jnp.where(good, row, 0.0) for row in rows[3:]]
            mis = n[0] * (p[0] - q[0]) + n[1] * (p[1] - q[1]) + n[2] * (p[2] - q[2])
            halves.append((cross(p, n) + n, cross(q, n) + n, mis))
        own_row = jnp.zeros((8, LANES), jnp.float32)
        far_row = jnp.zeros((8, LANES), jnp.float32)

        def total(make):
            acc = None
            for half in halves:
                acc = make(half) if acc is None else acc + make(half)
            return jnp.sum(acc, axis=1, keepdims=True)

        for f, (a, b) in enumerate(upper(6)):
            s = total(lambda v: v[0][a] * v[0][b])
            own_row = jnp.where(lane == PAIR * g + f, s, own_row)
            if a < 3:
                s = total(lambda v: v[1][a] * v[1][b])
            far_row = jnp.where(lane == f, s, far_row)
        for a in range(6):
            s = total(lambda v: v[0][a] * v[2])
            own_row = jnp.where(lane == PAIR * g + 21 + a, s, own_row)
            if a < 3:
                s = total(lambda v: v[1][a] * v[2])
            far_row = jnp.where(lane == 21 + a, -s, far_row)
        far[far_to, r0 : r0 + 8, :] = far_row
        return own_row

    def scatter(t, far_at):
        tot[...] += pick(scan == got_ids[t][:, :cap], far[far_at])

    far[1] = jnp.zeros(far.shape[1:], jnp.float32)

    def work(t, j):
        @pl.when(j > 0)
        def _():
            pts_copy(t, t).wait_recv()

        scatter(recv_at(jnp.maximum(j - 1, 0), me, tiles), (j + 1) % 2)
        for g in range(cap // 8):
            gather(t, g)

        @pl.when(j >= 0)
        def _():
            row = group(t, 0, j % 2)
            for g in range(1, cap // 8):
                row = row + group(t, g, j % 2)
            own[t] = row[:4] + pltpu.roll(row, LANES // 2, 1)[4:]

        @pl.when(j == 0)
        def _():
            back[grp * tiles + me] = own[t]

        @pl.when(j > 0)
        def _():
            own_copy(t, grp).start()

        own_copy(t, other).start()

    each(0, tiles, work, recv_at)
    scatter(recv_at(tiles - 1, me, tiles), (tiles - 1) % 2)
    seg_copy.wait_recv()
    all_of(pts, got, ps, pr.at[me], tiles - 1).wait_send()
    all_of(ids, got_ids, js, jr, tiles - 1).wait_send()
    seg_copy.wait_send()
    swap.start()
    wide = lax.broadcasted_iota(jnp.int32, (SCANS_DEV, tiles * 4), 0)
    groups = cap // 4
    for c, mine in enumerate((seg, seg_other)):
        for g in range(groups):
            here = wide == mine[g : g + 1, :]
            masks[c * groups + g] = here.astype(jnp.float32).astype(jnp.bfloat16)
    all_of(back, back, ss, rs, 2 * tiles - 1).wait_recv()
    sums = tot[...]
    for g in range(groups):
        for c, at in enumerate((grp, other)):
            rows = back[pl.ds(at * tiles, tiles)].reshape(tiles * 4, LANES)
            part = pick_by(masks[c * groups + g], rows)
            if g > 0:
                part = pltpu.roll(part, LANES - PAIR * (g // 2) - LANES // 2 * (g % 2), 1)
            sums = sums + part
    all_of(back, back, ss, rs, 2 * tiles - 1).wait_send()
    swap.wait()
    full = jnp.transpose(sums + partner[...])
    for a, row in enumerate(solve_rows([full[f : f + 1, :] for f in range(27)])):
        out[a : a + 1, :] = row


def solve_rows(rows):
    entries = {}
    for f, (a, b) in enumerate(upper(6)):
        entries[a, b] = rows[f]
    traced = entries[0, 0]
    for a in range(1, 6):
        traced = traced + entries[a, a]
    shift_by = DAMPING * traced / 6.0
    for a in range(6):
        entries[a, a] = entries[a, a] + shift_by
    values = [-rows[21 + a] for a in range(6)]
    for k in range(6):
        for a in range(k + 1, 6):
            factor = entries[k, a] / entries[k, k]
            for b in range(a, 6):
                entries[a, b] = entries[a, b] - factor * entries[k, b]
            values[a] = values[a] - factor * values[k]
    result = [None] * 6
    for a in range(5, -1, -1):
        running = values[a]
        for b in range(a + 1, 6):
            running = running - entries[a, b] * result[b]
        result[a] = running / entries[a, a]
    return result


def body(source_points, intersection, target_scan, matches, target_points, target_normals):
    tiles = lax.axis_size("tile")
    blocks = intersection.shape[1]
    points = source_points.shape[2] // blocks
    cap = -(-(2 * blocks // tiles) // 8) * 8
    f32, i32 = jnp.float32, jnp.int32
    shape = jax.ShapeDtypeStruct
    pts_t = (tiles, 4, cap, points)
    rows = (3, blocks * points // LANES, 1, LANES)
    ids_t, sums_t = (tiles, 1, LANES), (SCANS_DEV, LANES)
    return pl.pallas_call(
        main_kernel,
        out_shape=pltpu.VMEM((6, SCANS_DEV), f32),
        in_specs=[ANY] * 6,
        out_specs=VMEM,
        scratch_shapes=[
            pltpu.VMEM((1, blocks), i32),
            pltpu.VMEM((1, blocks), i32),
            pltpu.VMEM(rows, f32),
            pltpu.VMEM(rows[1:], i32),
            pltpu.VMEM(target_points.shape, f32),
            pltpu.VMEM(target_normals.shape, f32),
            pltpu.VMEM((cap // 8, tiles * 8), i32),
            pltpu.SMEM((cap // 8, tiles * 8), i32),
            pltpu.VMEM(ids_t, i32),
            pltpu.VMEM((cap // 4, tiles * 4), i32),
            pltpu.VMEM((cap // 4, tiles * 4), i32),
            pltpu.VMEM(pts_t, f32),
            pltpu.VMEM(pts_t, f32),
            pltpu.VMEM(ids_t, i32),
            pltpu.SMEM(ids_t, i32),
            pltpu.VMEM((SCANS_DEV, 8, TARGET_PTS - LANES), f32),
            pltpu.VMEM((cap // 8, points // LANES, TARGET_PTS // LANES - 1, 64, LANES), f32),
            pltpu.VMEM((tiles, 4, LANES), f32),
            pltpu.VMEM((2, cap, LANES), f32),
            pltpu.VMEM((2 * tiles, 4, LANES), f32),
            pltpu.VMEM(sums_t, f32),
            pltpu.VMEM(sums_t, f32),
            pltpu.VMEM((cap // 2, SCANS_DEV, tiles * 4), jnp.bfloat16),
        ]
        + [pltpu.SemaphoreType.DMA((tiles,))]
        + [pltpu.SemaphoreType.DMA] * 5
        + [pltpu.SemaphoreType.DMA((9,))]
        + [pltpu.SemaphoreType.DMA] * 4,
        compiler_params=pltpu.CompilerParams(collective_id=0, has_side_effects=True),
        name="main",
    )(
        intersection.reshape(1, blocks),
        target_scan,
        source_points.reshape(rows),
        matches.reshape(rows[1:]),
        target_points,
        target_normals,
    )


def solution(mesh):
    in_specs = (
        P("grp", None, "tile"),
        P("grp", "tile", None),
        P("grp", "tile"),
        P("grp", "tile"),
        P(None, "tile"),
        P(None, "tile"),
    )
    out_specs = P(None, "tile")
    return jax.shard_map(body, mesh=mesh, in_specs=in_specs, out_specs=out_specs, check_vma=False)
```

```python
import jax
import jax.numpy as jnp
from jax import lax
from jax.experimental import pallas as pl
from jax.experimental.pallas import tpu as pltpu
from jax.sharding import PartitionSpec as P

SCANS_DEV = 64
TARGET_PTS = 512
DAMPING = 0.1
LANES = 128
PAIR = 32
AHEAD = 2
MESH = pl.DeviceIdType.MESH
VMEM = pl.BlockSpec(memory_space=pltpu.VMEM)
ANY = pl.BlockSpec(memory_space=pl.ANY)


def spread(to, rows, wide):
    for g in range(to.shape[0]):
        to[g : g + 1, :] = jnp.concatenate(
            [rows[t : t + 1, g * wide : (g + 1) * wide] for t in range(rows.shape[0])], axis=1
        )


def plan(dest, chosen, block, ids, seg, ready):
    tiles = ids.shape[0]
    blocks = dest.shape[1]
    cap = seg.shape[0] * 4
    per_scan = blocks // SCANS_DEV
    f32 = jnp.float32
    hit = dest[...] == lax.broadcasted_iota(jnp.int32, (tiles, blocks), 0)
    first = lax.broadcasted_iota(jnp.int32, (blocks, blocks), 0)
    second = lax.broadcasted_iota(jnp.int32, (blocks, blocks), 1)
    rank = jnp.dot(
        hit.astype(f32), (first <= second).astype(f32), preferred_element_type=f32
    ).astype(jnp.int32)
    rank = jnp.where(hit, rank, 0)
    lane = lax.broadcasted_iota(jnp.int32, (tiles, LANES), 1)

    def listed(values):
        out = jnp.zeros((tiles, LANES), f32)
        for r in range(cap):
            value = jnp.sum(jnp.where(rank == r + 1, values, 0.0), axis=1, keepdims=True)
            out = jnp.where(lane == r, value, out)
        return out.astype(jnp.int32) - 1

    place = lax.broadcasted_iota(jnp.int32, (tiles, blocks), 1).astype(f32) + 1.0
    at = listed(place)
    spread(block, at, 8)
    ready()
    named = listed(chosen[...].astype(f32) + 1.0)
    scan = jnp.where(at >= 0, at // per_scan, -1)
    for t in range(tiles):
        ids[t] = named[t : t + 1]
    spread(seg, scan, 4)


def flip(me, k, tiles):
    other, bit = 0, 1
    while bit < tiles:
        other = other + (me // bit + k // bit) % 2 * bit
        bit *= 2
    return other


def send_at(j, me, tiles):
    half, quarter = tiles // 2, tiles // 4
    place = me // quarter
    inner = (place // 2 + place) % 2
    first = 6
    mixed = j - first
    is_far = (mixed <= 0) | ((mixed <= 2 * (half - first)) & (mixed % 2 == 1))
    i = jnp.where(mixed <= 0, jnp.maximum(j - 1, 0), first + (mixed - 1) // 2)
    n = jnp.where(mixed <= 2 * (half - first), mixed // 2, j - half)
    code = 3 - (inner * (1 - i // quarter) + (1 - inner) * (i % 2))
    low = inner * (i % quarter) + (1 - inner) * (i // 2)
    far = code * quarter + quarter - 1 - low
    return flip(me, jnp.where(is_far, far, half - n), tiles)


def recv_at(j, me, tiles):
    half, quarter = tiles // 2, tiles // 4
    place = me // quarter
    inner = (place // 2 + place) % 2
    last = j // (tiles - 1)
    i = j // 2 - 1 + last
    second = i // quarter
    code = 3 - (inner + second) % 2
    far = code * quarter + quarter - 1 - i % quarter
    near = (half - (j + 1) // 2) * jnp.minimum(j, 1)
    return flip(me, jnp.where((j > 0) & (j % 2 - last == 0), far, near), tiles)


def pick(here, rows):
    bf16, f32 = jnp.bfloat16, jnp.float32
    parts = []
    for _ in range(3):
        parts.append(rows.astype(bf16))
        rows = rows - parts[-1].astype(f32)
    here = here.astype(f32).astype(bf16)
    return jnp.dot(
        jnp.concatenate([here] * 3, axis=1),
        jnp.concatenate(parts, axis=0),
        preferred_element_type=f32,
    )


def cross(u, v):
    return [
        u[1] * v[2] - u[2] * v[1],
        u[2] * v[0] - u[0] * v[2],
        u[0] * v[1] - u[1] * v[0],
    ]


def upper(vec):
    return [(a, b) for a in range(6) for b in range(a, 6)]


def main_kernel(
    dest_in, chosen_in, sp_in, mt_in, tp_in, tn_in, out,
    dest, chosen, sp, mt, tp, tn, places, block, ids, seg,
    seg_other, pts, got, got_ids, named, table, picked, own, far, back, tot, partner,
    pr, ps, js, jr, ss, rs, ls, hs, hr, gs, gr,
):
    tiles, _, cap, points = pts.shape
    blocks = dest.shape[1]
    me = lax.axis_index("tile")
    grp = lax.axis_index("grp")
    other = 1 - grp
    barrier = pltpu.get_barrier_semaphore()

    def greet(k, c):
        to = lax.rem(me + k, tiles)
        for side in range(2):
            pl.semaphore_signal(
                barrier, inc=1, device_id={"grp": side, "tile": to}, device_id_type=MESH
            )
        return c

    pl.semaphore_signal(barrier, inc=1, device_id={"grp": other}, device_id_type=MESH)
    lax.fori_loop(1, tiles, greet, 0)
    loads = [
        pltpu.make_async_copy(src, dst, ls.at[i])
        for i, (src, dst) in enumerate(
            [(dest_in, dest), (chosen_in, chosen), (sp_in, sp), (mt_in, mt), (tp_in, tp), (tn_in, tn)]
        )
    ]
    for load in loads:
        load.start()

    def remote(src, dst, send, recv, to, side=grp):
        return pltpu.make_async_remote_copy(
            src, dst, send, recv, {"grp": side, "tile": to}, MESH
        )

    def id_copy(t):
        return remote(ids.at[t], got_ids.at[me], js, jr, t)

    def pts_copy(to, frm):
        return remote(pts.at[to], got.at[frm], ps, pr.at[frm], to)

    def own_copy(t, side):
        return remote(own.at[t], back.at[grp * tiles + me], ss, rs, t, side)

    def all_of(src, dst, send, recv, count):
        span = pl.ds(0, count)
        return remote(src.at[span], dst.at[span], send, recv, me, other)

    seg_copy = remote(seg, seg_other, hs, hr, me, other)
    swap = remote(tot, partner, gs, gr, me, other)

    def each(start, stop, act, at=send_at):
        def one(j, c):
            act(at(j, me, tiles), j)
            return c

        lax.fori_loop(start, stop, one, 0)

    def pack(t, to, at_to):
        for r in range(cap):
            b = block[r // 8, t * 8 + r % 8]
            used = jnp.minimum(b, 0) + 1
            for h in range(points // LANES):
                span = slice(h * LANES, (h + 1) * LANES)
                at = jnp.clip(b, 0, blocks - 1) * (points // LANES) + h
                for a in range(3):
                    to[at_to, a, r : r + 1, span] = sp[a, at]
                to[at_to, 3, r : r + 1, span] = (mt[at] * used + (used - 1)).astype(jnp.float32)

    loads[0].wait()
    loads[1].wait()
    to_smem = pltpu.make_async_copy(places, block, ls.at[6])
    plan(dest, chosen, places, ids, seg, to_smem.start)
    loads[2].wait()
    loads[3].wait()
    to_smem.wait()
    ahead = min(AHEAD, tiles - 1)
    each(1, ahead + 1, lambda t, j: pack(t, pts, t))
    pl.semaphore_wait(barrier, 2 * tiles - 1)
    each(1, tiles, lambda t, j: id_copy(t).start())
    each(1, ahead + 1, lambda t, j: pts_copy(t, me).start())
    seg_copy.start()

    def pack_send(t, j):
        @pl.when(j < tiles)
        def _():
            pack(t, pts, t)

        @pl.when(j > ahead + 1)
        def _():
            pts_copy(send_at(j - 1, me, tiles), me).start()

    each(ahead + 1, tiles + 1, pack_send)
    self_ids = pltpu.make_async_copy(ids.at[me], got_ids.at[me], ls.at[7])
    self_ids.start()
    pack(me, got, me)
    loads[4].wait()
    loads[5].wait()

    chunks = TARGET_PTS // LANES - 1

    def fill(s, c):
        def cols(q):
            return pl.ds(pl.multiple_of(s * TARGET_PTS + q * LANES, LANES), LANES)

        for q in range(chunks):
            span = slice(q * LANES, (q + 1) * LANES)
            table[s, 0:3, span] = tp[:, cols(q)]
            table[s, 3:6, span] = tn[:, cols(q)]
            for r in range(2):
                ref, a = ((tp, 2 * q + r), (tn, 2 * q + r - 3))[2 * q + r > 2]
                table[s, 6 + r : 7 + r, span] = ref[a : a + 1, cols(chunks)]
        return c

    lax.fori_loop(0, SCANS_DEV, fill, 0, unroll=4)
    tot[...] = jnp.zeros(tot.shape, jnp.float32)
    self_ids.wait()
    all_of(ids, got_ids, js, jr, tiles - 1).wait_recv()
    load_ids = pltpu.make_async_copy(got_ids, named, ls.at[8])
    load_ids.start()
    load_ids.wait()
    lane = lax.broadcasted_iota(jnp.int32, (8, LANES), 1)
    scan = lax.broadcasted_iota(jnp.int32, (SCANS_DEV, cap), 0)
    halves_of = points // LANES

    def gather(d, g):
        r0 = g * 8
        near = got[d, 3, r0 : r0 + 8, :].astype(jnp.int32)
        for j in range(8):
            tab = table.at[jnp.clip(named[d, 0, r0 + j], 0, SCANS_DEV - 1)]
            for h in range(halves_of):
                at = jnp.broadcast_to(near[j : j + 1, h * LANES : (h + 1) * LANES], (8, LANES))
                low = at & (LANES - 1)
                for q in range(chunks):
                    picked[g, h, q, j * 8 : j * 8 + 8, :] = jnp.take_along_axis(
                        tab[:, q * LANES : (q + 1) * LANES],
                        low,
                        axis=1,
                        mode="promise_in_bounds",
                    )

    def group(d, g, far_to):
        r0 = g * 8
        near = got[d, 3, r0 : r0 + 8, :].astype(jnp.int32)
        halves = []
        for h in range(halves_of):
            span = slice(h * LANES, (h + 1) * LANES)
            good = near[:, span] >= 0
            chunk = (near[:, span] >> 7) & chunks
            rows = []
            for a in range(6):
                row = picked[g, h, a // 2, pl.ds(6 + a % 2, 8, stride=8), :]
                for q in range(chunks):
                    row = jnp.where(chunk == q, picked[g, h, q, pl.ds(a, 8, stride=8), :], row)
                rows.append(row)
            p = [
                jnp.where(good, got[d, a, r0 : r0 + 8, span], 0.0) for a in range(3)
            ]
            q = rows[:3]
            n = [jnp.where(good, row, 0.0) for row in rows[3:]]
            mis = n[0] * (p[0] - q[0]) + n[1] * (p[1] - q[1]) + n[2] * (p[2] - q[2])
            halves.append((cross(p, n) + n, cross(q, n) + n, mis))
        own_row = jnp.zeros((8, LANES), jnp.float32)
        far_row = jnp.zeros((8, LANES), jnp.float32)

        def total(make):
            acc = None
            for half in halves:
                acc = make(half) if acc is None else acc + make(half)
            return jnp.sum(acc, axis=1, keepdims=True)

        for f, (a, b) in enumerate(upper(6)):
            s = total(lambda v: v[0][a] * v[0][b])
            own_row = jnp.where(lane == PAIR * g + f, s, own_row)
            if a < 3:
                s = total(lambda v: v[1][a] * v[1][b])
            far_row = jnp.where(lane == f, s, far_row)
        for a in range(6):
            s = total(lambda v: v[0][a] * v[2])
            own_row = jnp.where(lane == PAIR * g + 21 + a, s, own_row)
            if a < 3:
                s = total(lambda v: v[1][a] * v[2])
            far_row = jnp.where(lane == 21 + a, -s, far_row)
        far[far_to, r0 : r0 + 8, :] = far_row
        return own_row

    def scatter(t, far_at):
        tot[...] += pick(scan == got_ids[t][:, :cap], far[far_at])

    far[1] = jnp.zeros(far.shape[1:], jnp.float32)

    def work(t, j):
        @pl.when(j > 0)
        def _():
            pts_copy(t, t).wait_recv()

        scatter(recv_at(jnp.maximum(j - 1, 0), me, tiles), (j + 1) % 2)
        for g in range(cap // 8):
            gather(t, g)

        @pl.when(j >= 0)
        def _():
            row = group(t, 0, j % 2)
            for g in range(1, cap // 8):
                row = row + group(t, g, j % 2)
            own[t] = row[:4] + pltpu.roll(row, LANES // 2, 1)[4:]

        @pl.when(j == 0)
        def _():
            back[grp * tiles + me] = own[t]

        @pl.when(j > 0)
        def _():
            own_copy(t, grp).start()

        own_copy(t, other).start()

    each(0, tiles, work, recv_at)
    scatter(recv_at(tiles - 1, me, tiles), (tiles - 1) % 2)
    seg_copy.wait_recv()
    all_of(pts, got, ps, pr.at[me], tiles - 1).wait_send()
    all_of(ids, got_ids, js, jr, tiles - 1).wait_send()
    seg_copy.wait_send()
    swap.start()
    all_of(back, back, ss, rs, 2 * tiles - 1).wait_recv()
    sums = tot[...]
    wide = lax.broadcasted_iota(jnp.int32, (SCANS_DEV, tiles * 4), 0)
    for mine, at in ((seg, grp), (seg_other, other)):
        rows = back[pl.ds(at * tiles, tiles)].reshape(tiles * 4, LANES)
        for g in range(cap // 8):
            for h in range(2):
                part = pick(wide == mine[2 * g + h : 2 * g + h + 1, :], rows)
                if g + h > 0:
                    part = pltpu.roll(part, LANES - PAIR * g - LANES // 2 * h, 1)
                sums = sums + part
    all_of(back, back, ss, rs, 2 * tiles - 1).wait_send()
    swap.wait()
    full = jnp.transpose(sums + partner[...])
    for a, row in enumerate(solve_rows([full[f : f + 1, :] for f in range(27)])):
        out[a : a + 1, :] = row


def solve_rows(rows):
    entries = {}
    for f, (a, b) in enumerate(upper(6)):
        entries[a, b] = rows[f]
    traced = entries[0, 0]
    for a in range(1, 6):
        traced = traced + entries[a, a]
    shift_by = DAMPING * traced / 6.0
    for a in range(6):
        entries[a, a] = entries[a, a] + shift_by
    values = [-rows[21 + a] for a in range(6)]
    for k in range(6):
        for a in range(k + 1, 6):
            factor = entries[k, a] / entries[k, k]
            for b in range(a, 6):
                entries[a, b] = entries[a, b] - factor * entries[k, b]
            values[a] = values[a] - factor * values[k]
    result = [None] * 6
    for a in range(5, -1, -1):
        running = values[a]
        for b in range(a + 1, 6):
            running = running - entries[a, b] * result[b]
        result[a] = running / entries[a, a]
    return result


def body(source_points, intersection, target_scan, matches, target_points, target_normals):
    tiles = lax.axis_size("tile")
    blocks = intersection.shape[1]
    points = source_points.shape[2] // blocks
    cap = -(-(2 * blocks // tiles) // 8) * 8
    f32, i32 = jnp.float32, jnp.int32
    shape = jax.ShapeDtypeStruct
    pts_t = (tiles, 4, cap, points)
    rows = (3, blocks * points // LANES, 1, LANES)
    ids_t, sums_t = (tiles, 1, LANES), (SCANS_DEV, LANES)
    return pl.pallas_call(
        main_kernel,
        out_shape=pltpu.VMEM((6, SCANS_DEV), f32),
        in_specs=[ANY] * 6,
        out_specs=VMEM,
        scratch_shapes=[
            pltpu.VMEM((1, blocks), i32),
            pltpu.VMEM((1, blocks), i32),
            pltpu.VMEM(rows, f32),
            pltpu.VMEM(rows[1:], i32),
            pltpu.VMEM(target_points.shape, f32),
            pltpu.VMEM(target_normals.shape, f32),
            pltpu.VMEM((cap // 8, tiles * 8), i32),
            pltpu.SMEM((cap // 8, tiles * 8), i32),
            pltpu.VMEM(ids_t, i32),
            pltpu.VMEM((cap // 4, tiles * 4), i32),
            pltpu.VMEM((cap // 4, tiles * 4), i32),
            pltpu.VMEM(pts_t, f32),
            pltpu.VMEM(pts_t, f32),
            pltpu.VMEM(ids_t, i32),
            pltpu.SMEM(ids_t, i32),
            pltpu.VMEM((SCANS_DEV, 8, TARGET_PTS - LANES), f32),
            pltpu.VMEM((cap // 8, points // LANES, TARGET_PTS // LANES - 1, 64, LANES), f32),
            pltpu.VMEM((tiles, 4, LANES), f32),
            pltpu.VMEM((2, cap, LANES), f32),
            pltpu.VMEM((2 * tiles, 4, LANES), f32),
            pltpu.VMEM(sums_t, f32),
            pltpu.VMEM(sums_t, f32),
        ]
        + [pltpu.SemaphoreType.DMA((tiles,))]
        + [pltpu.SemaphoreType.DMA] * 5
        + [pltpu.SemaphoreType.DMA((9,))]
        + [pltpu.SemaphoreType.DMA] * 4,
        compiler_params=pltpu.CompilerParams(collective_id=0, has_side_effects=True),
        name="main",
    )(
        intersection.reshape(1, blocks),
        target_scan,
        source_points.reshape(rows),
        matches.reshape(rows[1:]),
        target_points,
        target_normals,
    )


def solution(mesh):
    in_specs = (
        P("grp", None, "tile"),
        P("grp", "tile", None),
        P("grp", "tile"),
        P("grp", "tile"),
        P(None, "tile"),
        P(None, "tile"),
    )
    out_specs = P(None, "tile")
    return jax.shard_map(body, mesh=mesh, in_specs=in_specs, out_specs=out_specs, check_vma=False)
```
